32 devices in a mesh: gx: 8 (over z, x), gy: 4 (over y, core).
Axes of the slice: x: 2, y: 2, z: 4, core: 2. Of those that a mesh axis runs over, the one named last changes fastest.
Arguments:
- clm_block: int32 [262144], P(('gx', 'gy')), may hold values from 0 to 31, as said below
- clm_cell: int32 [262144], P(('gx', 'gy')), may hold values from 0 to 8191, as said below
- precip: float32 [262144], P(('gx', 'gy')), may hold values from 0.05 to 2
- evap_demand: float32 [262144], P(('gx', 'gy')), may hold values from 0.05 to 1
- root_share: float32 [10, 262144], P(None, ('gx', 'gy')), may hold values from 0.05 to 1
- sat_before: float32 [10, 262144], P(None, ('gx', 'gy')), may hold values from 0.2 to 1
- pressure: float32 [10, 256, 1024], P(None, 'gx', 'gy'), may hold values from -3 to 0.5
- conductivity: float32 [10, 256, 1024], P(None, 'gx', 'gy'), may hold values from 0.1 to 3
- porosity: float32 [10, 256, 1024], P(None, 'gx', 'gy'), may hold values from 0.25 to 0.5
- freeze_state: int32 [10, 256, 1024], P(None, 'gx', 'gy'), may hold values from 0 to 2
- land_mask: int32 [256, 1024], P('gx', 'gy'), may hold values 0 or 1
Outputs:
- new_pressure: float32 [10, 256, 1024], P(None, 'gx', 'gy')
- returned_sat: float32 [10, 262144], P(None, ('gx', 'gy'))
The draws below stay inside these ranges and needn't reach their ends.
Inputs may be any that keep to these rules, and one draw needn't show every extreme that they name: Grid blocks are 32 x 256 columns, numbered with the second horizontal dimension fastest. Within one device's entries clm_block never falls; one device's entries name at most 384 columns of one block, and exactly that many for some blocks. `clm_cell`: together with clm_block, every grid column is named exactly once.
All inputs are finite; a program needn't handle non-finite values. No bound on the sum of `land_mask` on one device may be relied on, other than what follows from the above.
Results may differ from the reference program's by a relative error of at most 0.0002.
Values sent between devices are 32-bit elements; how exact they have to be, the bound alone decides.
No kernel may reach another device: no remote copies, remote signals or barrier semaphores. Data moves between devices by JAX's collectives and lax.ppermute only.
A program may use at most 64 MiB of HBM per device.

```python
import math
import jax
import jax.numpy as jnp
from jax import lax

NZ = 10
CX = 32
CY = 256
NEWTON = 2
SWEEPS = 4
NX = 256
NY = 1024
COLS = 262144
N_GX = 8
N_GY = 4


def column_places(key):
    devices = N_GX * N_GY
    block_cells = CX * CY
    average = block_cells // devices
    swing = average // 2
    base_key = jax.random.fold_in(key, 7)
    first_key, second_key = jax.random.split(base_key, 2)
    order = jax.random.permutation(first_key, devices)
    signs = jnp.where(order < devices // 2, 1, -1).astype(jnp.int32)
    senders = jnp.arange(devices, dtype=jnp.int32)[:, None]
    owners = jnp.arange(devices, dtype=jnp.int32)[None, :]
    counts = average + swing * signs[(owners - senders) % devices]
    offsets = jnp.cumsum(counts, axis=0) - counts
    places = jax.vmap(lambda single: jax.random.permutation(single, block_cells))(jax.random.split(second_key, devices))

    def one_sender(sender):
        row_counts = counts[sender]
        owner = jnp.repeat(jnp.arange(devices, dtype=jnp.int32), row_counts, total_repeat_length=block_cells)
        starts = jnp.cumsum(row_counts) - row_counts
        ranks = jnp.arange(block_cells, dtype=jnp.int32) - starts[owner]
        local_cell = places[owner, offsets[sender, owner] + ranks]
        return (owner.astype(jnp.int32), local_cell.astype(jnp.int32))
    owner_all, cell_all = lax.map(one_sender, jnp.arange(devices, dtype=jnp.int32))
    return (owner_all.reshape(-1).astype(jnp.int32), cell_all.reshape(-1).astype(jnp.int32))


def draw_clm_block(key, part):
    return column_places(key)[0]


def draw_clm_cell(key, part):
    return column_places(key)[1]


def with_ends(drawn, own_key, low, top_value):
    longest = drawn.shape.index(max(drawn.shape))
    spots = []
    for shift in (0, 1):
        where = [jax.random.randint(jax.random.fold_in(own_key, axis), (), 0, length) for axis, length in enumerate(drawn.shape)]
        where[longest] = (where[longest] + shift) % drawn.shape[longest]
        spots.append(tuple(where))
    return drawn.at[spots[0]].set(low).at[spots[1]].set(top_value)


def level_of(own_key, shape, cuts, smallest, largest):
    def one(axis_at, parts):
        steps = jax.random.uniform(jax.random.fold_in(jax.random.fold_in(own_key, 6), axis_at), (parts,), jnp.float32, smallest / len(cuts), largest / len(cuts))
        return jnp.repeat(jnp.exp(steps), shape[axis_at] // parts).reshape((-1,) + (1,) * (len(shape) - axis_at - 1))

    loudness = one(*cuts[0])
    for cut in cuts[1:]:
        loudness = loudness * one(*cut)
    return loudness


def setup_inputs(seed: int = 0) -> dict:
    arg_keys = jax.random.split(jax.random.key(seed), 12)
    return {
        "clm_block": draw_clm_block(jax.random.fold_in(arg_keys[11], 71), 0),
        "clm_cell": draw_clm_cell(jax.random.fold_in(arg_keys[11], 71), 0),
        "precip": jnp.clip(jnp.exp(math.log(2.0) - 3.6888794 * jax.random.uniform(arg_keys[2], (COLS,), jnp.float32) ** level_of(arg_keys[2], (COLS,), ((0, 32),), -0.2, 0.2)), 0.05, 2.0),
        "evap_demand": jnp.clip(jnp.exp(math.log(1.0) - 2.9957323 * jax.random.uniform(arg_keys[3], (COLS,), jnp.float32) ** level_of(arg_keys[3], (COLS,), ((0, 32),), -0.2, 0.2)), 0.05, 1.0),
        "root_share": jnp.clip(0.05 + 0.95 * jax.random.uniform(arg_keys[4], (NZ, COLS), jnp.float32) ** level_of(arg_keys[4], (NZ, COLS), ((1, 32),), -0.2, 0.2), 0.05, 1.0),
        "sat_before": jnp.clip(0.2 + 0.8 * jax.random.uniform(arg_keys[5], (NZ, COLS), jnp.float32) ** level_of(arg_keys[5], (NZ, COLS), ((1, 32),), -0.2, 0.2), 0.2, 1.0),
        "pressure": jnp.clip(-3.0 + 3.5 * jax.random.uniform(arg_keys[6], (NZ, NX, NY), jnp.float32) ** level_of(arg_keys[6], (NZ, NX, NY), ((1, 8), (2, 4)), -0.2, 0.2), -3.0, 0.5),
        "conductivity": jnp.clip(jnp.exp(math.log(3.0) - 3.4011974 * jax.random.uniform(arg_keys[7], (NZ, NX, NY), jnp.float32) ** level_of(arg_keys[7], (NZ, NX, NY), ((1, 8), (2, 4)), -0.2, 0.2)), 0.1, 3.0),
        "porosity": jnp.clip(0.25 + 0.25 * jax.random.uniform(arg_keys[8], (NZ, NX, NY), jnp.float32) ** level_of(arg_keys[8], (NZ, NX, NY), ((1, 8), (2, 4)), -0.2, 0.2), 0.25, 0.5),
        "freeze_state": with_ends(jax.random.randint(arg_keys[9], (NZ, NX, NY), 0, 3), jax.random.fold_in(arg_keys[9], 1), 0, 2).astype(jnp.int32),
        "land_mask": with_ends((jax.random.randint(arg_keys[10], (NX, NY), 0, 4) < 3).astype(jnp.int32), jax.random.fold_in(arg_keys[10], 1), 0, 1),
    }


OMEGA = 0.8
SIDE_CUTS = ((slice(0, -2), slice(1, -1)), (slice(2, None), slice(1, -1)), (slice(1, -1), slice(0, -2)), (slice(1, -1), slice(2, None)))

def saturation(field):
    dryness = jnp.maximum(-field, 0.0)
    return 1.0 / jnp.sqrt(1.0 + dryness * dryness)

def saturation_slope(field):
    dryness = jnp.maximum(-field, 0.0)
    inverse = 1.0 / jnp.sqrt(1.0 + dryness * dryness)
    return dryness * inverse * inverse * inverse

def frozen_factor(freeze_state):
    return jnp.where(freeze_state == 0, 1.0, jnp.where(freeze_state == 1, 0.2, 0.02)).astype(jnp.float32)

def mean_face(perm_one, perm_two, rel_one, rel_two):
    return perm_one * perm_two / (perm_one + perm_two) * (rel_one + rel_two)

def column_fluxes(precip, evap_demand, root_share, sat_before):
    weights = root_share * sat_before * sat_before
    total = 0.25 + lax.optimization_barrier(jnp.sum(weights, axis=0))
    uptake = evap_demand * weights / total
    infiltration = precip * (1.0 - sat_before[0] ** 3)
    topmost = jnp.concatenate([infiltration[None], jnp.zeros_like(uptake[1:])], axis=0)
    return topmost - uptake

def linearize(pressure_pad, perm_pad, stored_before, porosity, source):
    relative = saturation(pressure_pad) ** 3
    perm_mid = perm_pad[:, 1:-1, 1:-1]
    rel_mid = relative[:, 1:-1, 1:-1]
    middle = pressure_pad[:, 1:-1, 1:-1]
    sides = []
    lateral = jnp.zeros_like(middle)
    for first_cut, second_cut in SIDE_CUTS:
        side = mean_face(perm_mid, perm_pad[:, first_cut, second_cut], rel_mid, relative[:, first_cut, second_cut])
        sides.append(side)
        lateral = lateral + side * (middle - pressure_pad[:, first_cut, second_cut])
    vertical = mean_face(perm_mid[:-1], perm_mid[1:], rel_mid[:-1], rel_mid[1:])
    drainage = perm_mid[-1] * rel_mid[-1]
    zero_layer = jnp.zeros_like(middle[:1])
    down_flow = vertical * (middle[:-1] - middle[1:] + 1.0)
    outflow = jnp.concatenate([down_flow, drainage[None]], axis=0) - jnp.concatenate([zero_layer, down_flow], axis=0)
    residual = porosity * (saturation(middle) - stored_before) + lateral + outflow - source
    diagonal = porosity * saturation_slope(middle) + sides[0] + sides[1] + sides[2] + sides[3]
    diagonal = diagonal + jnp.concatenate([vertical, zero_layer], axis=0) + jnp.concatenate([zero_layer, vertical], axis=0)
    return (residual, diagonal, sides, vertical)

def neighbour_sum(field_pad, sides, vertical):
    total = jnp.zeros_like(sides[0])
    for side, cuts in zip(sides, SIDE_CUTS):
        total = total + side * field_pad[:, cuts[0], cuts[1]]
    middle = field_pad[:, 1:-1, 1:-1]
    zero_layer = jnp.zeros_like(middle[:1])
    below = jnp.concatenate([vertical * middle[1:], zero_layer], axis=0)
    above = jnp.concatenate([zero_layer, vertical * middle[:-1]], axis=0)
    return total + below + above

def pad_sides(field):
    return jnp.pad(field, ((0, 0), (1, 1), (1, 1)))

def reference(clm_block, clm_cell, precip, evap_demand, root_share, sat_before, pressure, conductivity, porosity, freeze_state, land_mask):
    grid_x = clm_block // N_GY * CX + clm_cell // CY
    grid_y = clm_block % N_GY * CY + clm_cell % CY
    clm_target = (grid_x * NY + grid_y).astype(jnp.int32)
    flux = column_fluxes(precip, evap_demand, root_share, sat_before)
    source = jnp.zeros((NZ, NX * NY), jnp.float32).at[:, clm_target].set(flux)
    source = source.reshape(NZ, NX, NY) * land_mask.astype(jnp.float32)[None]
    perm = conductivity * frozen_factor(freeze_state)
    perm_pad = pad_sides(perm)
    stored_before = saturation(pressure)
    pressure_now = pressure
    for newton_step in range(NEWTON):
        residual, diagonal, sides, vertical = linearize(pad_sides(pressure_now), perm_pad, stored_before, porosity, source)
        update = OMEGA * -residual / diagonal
        for sweep_turn in range(SWEEPS - 1):
            coupled = neighbour_sum(pad_sides(update), sides, vertical)
            update = update + OMEGA * (coupled - residual - diagonal * update) / diagonal
        pressure_now = pressure_now + update
    saturated = saturation(pressure_now).reshape(NZ, NX * NY)
    returned_sat = saturated[:, clm_target]
    return (pressure_now, returned_sat)
```

```python
import jax
import jax.numpy as jnp
from jax import lax
from jax.experimental import pallas as pl
from jax.experimental.pallas import tpu as pltpu
from jax.sharding import PartitionSpec as P

NEWTON = 2
SWEEPS = 4
OMEGA = 0.8
LANES = 128
ROWS = 8
HALO = 8
GROUPS = LANES // HALO


def params():
    return pltpu.CompilerParams(vmem_limit_bytes=48 * 2**20)


def saturation(field):
    dryness = jnp.maximum(-field, 0.0)
    return lax.rsqrt(1.0 + dryness * dryness)


def frozen_factor(freeze_state):
    return jnp.where(freeze_state == 0, 1.0, jnp.where(freeze_state == 1, 0.2, 0.02)).astype(
        jnp.float32
    )


def window_tiles(capacity):
    return capacity // LANES


def dispatch_kernel(layers, devices, capacity):
    chunks = window_tiles(capacity)
    fields = layers + 1

    def kernel(starts, block, cell, precip, evap, root, sat, out, packed):
        columns = root.shape[1]
        rows_of = 4 * LANES

        def flux(tile, carry):
            span = pl.ds(pl.multiple_of(tile * LANES, LANES), LANES)
            s = sat[:, span]
            w = root[:, span] * s * s
            total = 0.25 + jnp.sum(w, axis=0, keepdims=True)
            uptake = w * (evap[pl.ds(tile, 1), :] / total)
            top = s[0:1]
            rain = precip[pl.ds(tile, 1), :] * (1.0 - top * top * top)
            packed[0:1, span] = rain - uptake[0:1]
            packed[1:layers, span] = -uptake[1:]
            packed[layers:fields, span] = cell[pl.ds(tile, 1), :].astype(jnp.float32)
            return carry

        lax.fori_loop(0, columns // LANES, flux, 0, unroll=8)
        lane = lax.broadcasted_iota(jnp.int32, (1, LANES), 1)

        def window(owner, carry):
            start = starts[owner]
            count = starts[owner + 1] - start
            base = pl.multiple_of((start // LANES) * LANES, LANES)
            shift = start % LANES
            near = lane < LANES - shift
            turned = [
                pltpu.roll(packed[:, pl.ds(base + t * LANES, LANES)], LANES - shift, 1)
                for t in range(chunks + 1)
            ]
            for t in range(chunks):
                moved = jnp.where(near, turned[t], turned[t + 1])
                row = (owner * chunks + t) * fields
                held = t * LANES + lane < count
                out[pl.ds(row, layers), :] = moved[0:layers]
                out[pl.ds(row + layers, 1), :] = jnp.where(held, moved[layers:fields], -1.0)
            return carry

        lax.fori_loop(0, devices, window, 0, unroll=4)

    return kernel


def dispatch(starts, block, cell, precip, evap, root, sat, devices, capacity):
    layers, columns = root.shape
    fields = layers + 1
    rows = devices * window_tiles(capacity) * fields
    vmem = pl.BlockSpec(memory_space=pltpu.VMEM)
    fold = (columns // LANES, LANES)
    return pl.pallas_call(
        dispatch_kernel(layers, devices, capacity),
        out_shape=jax.ShapeDtypeStruct((rows, LANES), jnp.float32),
        in_specs=[pl.BlockSpec(memory_space=pltpu.SMEM)] + [vmem] * 6,
        out_specs=vmem,
        scratch_shapes=[pltpu.VMEM((2 * ROWS, columns + capacity + LANES), jnp.float32)],
        compiler_params=params(),
        name="dispatch",
    )(
        starts,
        block.reshape(fold),
        cell.reshape(fold),
        precip.reshape(fold),
        evap.reshape(fold),
        root,
        sat,
    )


def scatter_kernel(layers, cells_x, cells_y, batch):
    fields = layers + 1
    half = layers * cells_x

    def kernel(incoming, mask, out, low, high, total, spread):
        chunks = incoming.shape[0] // fields
        total[...] = jnp.zeros_like(total)
        row_x = lax.broadcasted_iota(jnp.int32, (cells_x, LANES), 0)
        row_y = lax.broadcasted_iota(jnp.int32, (cells_y, LANES), 0)

        def step(i, carry):
            onehots = []
            for b in range(batch):
                first = (i * batch + b) * fields
                cell = incoming[pl.ds(first + layers, 1), :].astype(jnp.int32)
                x = cell // cells_y
                y = cell - x * cells_y
                x = jnp.where(cell < 0, -1, x)
                onehots.append((row_y == y).astype(jnp.float32).astype(jnp.bfloat16))
                here = row_x == x
                values = incoming[pl.ds(first, layers), :]
                big = values.astype(jnp.bfloat16).astype(jnp.float32)
                small = values - big
                span = slice(b * LANES, (b + 1) * LANES)
                for k in range(layers):
                    rows = slice(k * cells_x, (k + 1) * cells_x)
                    spread[rows, span] = jnp.where(here, big[k : k + 1], 0.0).astype(jnp.bfloat16)
                    rows = slice(half + k * cells_x, half + (k + 1) * cells_x)
                    spread[rows, span] = jnp.where(here, small[k : k + 1], 0.0).astype(
                        jnp.bfloat16
                    )
            onehot = jnp.concatenate(onehots, axis=1)
            total[...] += lax.dot_general(
                spread[...],
                onehot,
                (((1,), (1,)), ((), ())),
                preferred_element_type=jnp.float32,
            )
            return carry

        lax.fori_loop(0, chunks // batch, step, 0)
        land = mask[...].astype(jnp.float32)
        for k in range(layers):
            rows = slice(k * cells_x, (k + 1) * cells_x)
            lower = slice(half + k * cells_x, half + (k + 1) * cells_x)
            source = (total[rows, :] + total[lower, :]) * land
            out[k] = source
            low[k] = source[:HALO]
            high[k] = source[cells_x - HALO :]

    return kernel


def scatter(incoming, mask, layers, cells_x, cells_y):
    chunks = incoming.shape[0] // (layers + 1)
    batch = max(b for b in (8, 6, 4, 3, 2, 1) if chunks % b == 0)
    strip = jax.ShapeDtypeStruct((layers, HALO, cells_y), jnp.float32)
    vmem = pl.BlockSpec(memory_space=pltpu.VMEM)
    return pl.pallas_call(
        scatter_kernel(layers, cells_x, cells_y, batch),
        out_shape=(jax.ShapeDtypeStruct((layers, cells_x, cells_y), jnp.float32), strip, strip),
        in_specs=[vmem, vmem],
        out_specs=(vmem, vmem, vmem),
        scratch_shapes=[
            pltpu.VMEM((2 * layers * cells_x, cells_y), jnp.float32),
            pltpu.VMEM((2 * layers * cells_x, batch * LANES), jnp.bfloat16),
        ],
        compiler_params=params(),
        name="scatter",
    )(incoming, mask)


def both_ways(low_end, high_end, axis):
    count = lax.axis_size(axis)
    forward = [(i, i + 1) for i in range(count - 1)]
    backward = [(target, source) for source, target in forward]
    return lax.ppermute(high_end, axis, forward), lax.ppermute(low_end, axis, backward)


def packed_rows(layers, cells_x):
    tiles = layers * (cells_x + 2 * HALO) // ROWS
    return -(-tiles // GROUPS) * ROWS


def tile_places(layers, cells_x):
    tiles = (cells_x + 2 * HALO) // ROWS
    for index in range(layers * tiles):
        yield index // tiles, index % tiles, index // GROUPS, index % GROUPS


def pack_kernel(layers, cells_x, cells_y):
    lane_of = lambda: lax.broadcasted_iota(jnp.int32, (ROWS, LANES), 1)

    def kernel(middle, below, above, left, right):
        fields = middle.shape[0]
        lane = lane_of()
        last = cells_x // ROWS + 1

        def column(f, k, t, cols):
            if t == 0:
                return below[f, k, :, cols]
            if t == last:
                return above[f, k, :, cols]
            return middle[f, k, (t - 1) * ROWS : t * ROWS, cols]

        for f in range(fields):
            for out, cols, offset in (
                (left, slice(0, LANES), 0),
                (right, slice(cells_y - LANES, cells_y), LANES - HALO),
            ):
                held = {}
                for k, t, place, group in tile_places(layers, cells_x):
                    tile = column(f, k, t, cols)
                    turn = (group * HALO - offset) % LANES
                    tile = pltpu.roll(tile, turn, 1) if turn else tile
                    if group == 0:
                        held[place] = tile
                    else:
                        here = (lane >= group * HALO) & (lane < (group + 1) * HALO)
                        held[place] = jnp.where(here, tile, held[place])
                for place, tile in held.items():
                    out[f, place * ROWS : (place + 1) * ROWS, :] = tile

    return kernel


def pack(middle, below, above):
    fields, layers, cells_x, cells_y = middle.shape
    out = jax.ShapeDtypeStruct((fields, packed_rows(layers, cells_x), LANES), jnp.float32)
    vmem = pl.BlockSpec(memory_space=pltpu.VMEM)
    return pl.pallas_call(
        pack_kernel(layers, cells_x, cells_y),
        out_shape=(out, out),
        in_specs=[vmem] * 3,
        out_specs=(vmem, vmem),
        compiler_params=params(),
        name="pack",
    )(middle, below, above)


def prepare_kernel(conductivity, freeze, porosity, pressure, out, low, high):
    cells_x = out.shape[2]
    perm = conductivity[...] * frozen_factor(freeze[...])
    for f, value in enumerate((perm, porosity[...], pressure[...])):
        out[f] = value
        low[f] = value[:, :HALO]
        high[f] = value[:, cells_x - HALO :]


def prepare(conductivity, freeze, porosity, pressure):
    layers, cells_x, cells_y = pressure.shape
    strip = jax.ShapeDtypeStruct((3, layers, HALO, cells_y), jnp.float32)
    vmem = pl.BlockSpec(memory_space=pltpu.VMEM)
    return pl.pallas_call(
        prepare_kernel,
        out_shape=(jax.ShapeDtypeStruct((3, layers, cells_x, cells_y), jnp.float32), strip, strip),
        in_specs=[vmem] * 4,
        out_specs=(vmem,) * 3,
        compiler_params=params(),
        name="prepare",
    )(conductivity, freeze, porosity, pressure)


def gather_slots(incoming, table, reply, layers, cells_x, cells_y):
    fields = layers + 1
    chunks = incoming.shape[0] // fields
    sub = lax.broadcasted_iota(jnp.int32, (ROWS, LANES), 0)
    across = cells_y // LANES
    groups = cells_x // ROWS * across

    def body(c, carry):
        cell = incoming[pl.ds(c * fields + layers, 1), :].astype(jnp.int32)
        cell = jnp.broadcast_to(jnp.maximum(cell, 0), (ROWS, LANES))
        x = cell // cells_y
        y = cell - x * cells_y
        lane = y % LANES
        group = (x // ROWS) * across + y // LANES
        wanted = x % ROWS == sub
        rows = []
        for k in range(layers):
            value = jnp.zeros((ROWS, LANES), jnp.float32)
            for g in range(groups):
                first = HALO + g // across * ROWS
                tile = table[k, first : first + ROWS, g % across * LANES : (g % across + 1) * LANES]
                found = jnp.take_along_axis(tile, lane, axis=1, mode="promise_in_bounds")
                value = jnp.where(group == g, found, value)
            value = jnp.where(wanted, value, 0.0)
            rows.append(jnp.sum(value, axis=0, keepdims=True))
        reply[pl.ds(c * layers, layers), :] = jnp.concatenate(rows, axis=0)
        return carry

    lax.fori_loop(0, chunks, body, 0, unroll=2)


def newton_kernel(layers, cells_x, cells_y):
    high_x = cells_x + 2 * HALO
    wide = cells_y + LANES

    def up(v):
        return pltpu.roll(v, high_x - 1, 0)

    def down(v):
        return pltpu.roll(v, 1, 0)

    def right(v):
        return pltpu.roll(v, wide - 1, 1)

    def left(v):
        return pltpu.roll(v, 1, 1)

    def kernel(
        fixed, fixed_low, fixed_high, fixed_left, fixed_right,
        src, src_low, src_high, src_left, src_right, incoming,
        new_pressure, reply,
        perm, poro, source, pres, stored,
        tx, ty, tz, rel, gz, flow,
        ax, bx, ay, by, az, bz, resid, update,
    ):
        lane = lax.broadcasted_iota(jnp.int32, (ROWS, LANES), 1)
        last = cells_x // ROWS + 1

        def widen(dest, field, middle, low, high, side_left, side_right):
            dest[:, HALO : HALO + cells_x, :cells_y] = middle[field]
            dest[:, :HALO, :cells_y] = low[field]
            dest[:, HALO + cells_x :, :cells_y] = high[field]
            for k, t, place, group in tile_places(layers, cells_x):
                rows = slice(place * ROWS, (place + 1) * ROWS)
                turn = (LANES - HALO - group * HALO) % LANES
                a = side_left[field, rows, :]
                a = pltpu.roll(a, turn, 1) if turn else a
                turn = (-group * HALO) % LANES
                b = side_right[field, rows, :]
                b = pltpu.roll(b, turn, 1) if turn else b
                tile = jnp.where(lane < HALO, b, jnp.where(lane >= LANES - HALO, a, 0.0))
                dest[k, t * ROWS : (t + 1) * ROWS, cells_y:] = tile

        widen(perm, 0, fixed, fixed_low, fixed_high, fixed_left, fixed_right)
        widen(poro, 1, fixed, fixed_low, fixed_high, fixed_left, fixed_right)
        widen(pres, 2, fixed, fixed_low, fixed_high, fixed_left, fixed_right)
        widen(source, 0, src, src_low, src_high, src_left, src_right)

        def face(a, b):
            joined = a + b
            return a * b / jnp.where(joined > 0.0, joined, 1.0)

        def still(k, carry):
            a = perm[k]
            tx[k] = face(a, up(a))
            ty[k] = face(a, right(a))
            tz[k] = face(a, perm[jnp.minimum(k + 1, layers - 1)])
            stored[k] = saturation(pres[k])
            return carry

        lax.fori_loop(0, layers, still, 0)

        for newton_step in range(NEWTON):

            def relative(k, carry):
                s = saturation(pres[k])
                rel[k] = s * s * s
                return carry

            lax.fori_loop(0, layers, relative, 0)

            def vertical(k, carry):
                r = rel[k]
                below = jnp.minimum(k + 1, layers - 1)
                g = tz[k] * (r + rel[below])
                inside = k < layers - 1
                g = jnp.where(inside, g, 0.0)
                gz[k + 1] = g
                drained = perm[k] * r
                flow[k + 1] = jnp.where(inside, g * (pres[k] - pres[below] + 1.0), drained)
                return carry

            gz[0] = jnp.zeros((high_x, wide), jnp.float32)
            flow[0] = jnp.zeros((high_x, wide), jnp.float32)
            lax.fori_loop(0, layers, vertical, 0)

            def linear(k, carry):
                p = pres[k]
                r = rel[k]
                gx = tx[k] * (r + up(r))
                gy = ty[k] * (r + right(r))
                fx = gx * (p - up(p))
                fy = gy * (p - right(p))
                gxd = down(gx)
                gyd = left(gy)
                s = saturation(p)
                porous = poro[k]
                residual = porous * (s - stored[k])
                residual = residual + (fx - down(fx)) + (fy - left(fy))
                residual = residual + (flow[k + 1] - flow[k]) - source[k]
                gzd = gz[k]
                gzu = gz[k + 1]
                diagonal = porous * (jnp.maximum(-p, 0.0) * r)
                diagonal = diagonal + (gx + gxd) + (gy + gyd) + (gzu + gzd)
                diagonal = jnp.where(diagonal > 0.0, diagonal, 1.0)
                scale = OMEGA / diagonal
                ax[k] = scale * gx
                bx[k] = scale * gxd
                ay[k] = scale * gy
                by[k] = scale * gyd
                az[k] = scale * gzu
                bz[k] = scale * gzd
                residual = scale * residual
                resid[k] = residual
                update[0, k] = -residual
                return carry

            lax.fori_loop(0, layers, linear, 0)

            for sweep in range(SWEEPS - 1):
                old = sweep % 2
                new = 1 - old

                def smooth(k, carry):
                    u = update[old, k]
                    v = (1.0 - OMEGA) * u - resid[k]
                    v = v + ax[k] * up(u) + bx[k] * down(u)
                    v = v + ay[k] * right(u) + by[k] * left(u)
                    v = v + az[k] * update[old, jnp.minimum(k + 1, layers - 1)]
                    v = v + bz[k] * update[old, jnp.maximum(k - 1, 0)]
                    update[new, k] = v
                    if sweep == SWEEPS - 2:
                        pres[k] = pres[k] + v
                    return carry

                lax.fori_loop(0, layers, smooth, 0)

        def finish(k, carry):
            p = pres[k, HALO : HALO + cells_x, :cells_y]
            new_pressure[k] = p
            rel[k, HALO : HALO + cells_x, :cells_y] = saturation(p)
            return carry

        lax.fori_loop(0, layers, finish, 0)
        gather_slots(incoming, rel, reply, layers, cells_x, cells_y)

    return kernel


def newton(fixed, source, incoming, layers, cells_x, cells_y):
    chunks = incoming.shape[0] // (layers + 1)
    high_x, wide = cells_x + 2 * HALO, cells_y + LANES
    field = pltpu.VMEM((layers, high_x, wide), jnp.float32)
    taller = pltpu.VMEM((layers + 1, high_x, wide), jnp.float32)
    vmem = pl.BlockSpec(memory_space=pltpu.VMEM)
    return pl.pallas_call(
        newton_kernel(layers, cells_x, cells_y),
        out_shape=(
            jax.ShapeDtypeStruct((layers, cells_x, cells_y), jnp.float32),
            jax.ShapeDtypeStruct((chunks * layers, LANES), jnp.float32),
        ),
        in_specs=[vmem] * 11,
        out_specs=(vmem, vmem),
        scratch_shapes=[field] * 5
        + [field] * 4
        + [taller] * 2
        + [field] * 7
        + [pltpu.VMEM((2, layers, high_x, wide), jnp.float32)],
        compiler_params=params(),
        name="newton",
    )(*fixed, *source, incoming)


def combine_kernel(layers, devices, capacity):
    chunks = window_tiles(capacity)

    def kernel(starts, answer, out, wide):
        lane = lax.broadcasted_iota(jnp.int32, (1, LANES), 1)

        def window(owner, carry):
            start = starts[owner]
            base = pl.multiple_of((start // LANES) * LANES, LANES)
            shift = start % LANES
            before = lane < shift
            row = owner * chunks * layers
            kept = wide[0:layers, pl.ds(base, LANES)]
            for t in range(chunks):
                turned = pltpu.roll(answer[pl.ds(row + t * layers, layers), :], shift, 1)
                wide[0:layers, pl.ds(base + t * LANES, LANES)] = jnp.where(before, kept, turned)
                kept = turned
            wide[0:layers, pl.ds(base + chunks * LANES, LANES)] = kept
            return carry

        lax.fori_loop(0, devices, window, 0)
        out[...] = wide[0:layers, : out.shape[1]]

    return kernel


def combine(starts, answer, layers, columns, devices, capacity):
    vmem = pl.BlockSpec(memory_space=pltpu.VMEM)
    return pl.pallas_call(
        combine_kernel(layers, devices, capacity),
        out_shape=jax.ShapeDtypeStruct((layers, columns), jnp.float32),
        in_specs=[pl.BlockSpec(memory_space=pltpu.SMEM), vmem],
        out_specs=vmem,
        scratch_shapes=[pltpu.VMEM((2 * ROWS, columns + capacity + LANES), jnp.float32)],
        compiler_params=params(),
        name="combine",
    )(starts, answer)


def on_device(
    clm_block,
    clm_cell,
    precip,
    evap_demand,
    root_share,
    sat_before,
    pressure,
    conductivity,
    porosity,
    freeze_state,
    land_mask,
):
    axes = ("gx", "gy")
    layers, columns = root_share.shape
    devices = lax.axis_size("gx") * lax.axis_size("gy")
    cells_x, cells_y = pressure.shape[1], pressure.shape[2]
    per_pair = columns // devices
    capacity = -(-(per_pair + per_pair // 2) // LANES) * LANES
    owners = jnp.arange(devices + 1, dtype=jnp.int32)
    starts = jnp.sum((clm_block[None, :] < owners[:, None]).astype(jnp.int32), axis=1)

    outgoing = dispatch(
        starts, clm_block, clm_cell, precip, evap_demand, root_share, sat_before, devices, capacity
    )
    flat = lax.all_to_all(outgoing.reshape(-1), axes, split_axis=0, concat_axis=0, tiled=True)
    incoming = flat.reshape(outgoing.shape)

    fixed, low, high = prepare(conductivity, freeze_state, porosity, pressure)
    below, above = both_ways(low, high, "gx")
    to_left, to_right = pack(fixed, below, above)
    side_left, side_right = both_ways(to_left, to_right, "gy")
    fixed = (fixed, below, above, side_left, side_right)

    source, low, high = scatter(incoming, land_mask, layers, cells_x, cells_y)
    below, above = both_ways(low, high, "gx")
    source, below, above = source[None], below[None], above[None]
    to_left, to_right = pack(source, below, above)
    side_left, side_right = both_ways(to_left, to_right, "gy")
    source = (source, below, above, side_left, side_right)

    new_pressure, reply = newton(fixed, source, incoming, layers, cells_x, cells_y)
    flat = lax.all_to_all(reply.reshape(-1), axes, split_axis=0, concat_axis=0, tiled=True)
    returned = combine(starts, flat.reshape(reply.shape), layers, columns, devices, capacity)
    return (new_pressure, returned)


def solution(mesh):
    columns = P(("gx", "gy"))
    layered = P(None, ("gx", "gy"))
    grid = P(None, "gx", "gy")
    return jax.shard_map(
        on_device,
        mesh=mesh,
        in_specs=(columns,) * 4 + (layered,) * 2 + (grid,) * 4 + (P("gx", "gy"),),
        out_specs=(grid, layered),
        check_vma=False,
    )
```

```python
import jax
import jax.numpy as jnp
from jax import lax
from jax.experimental import pallas as pl
from jax.experimental.pallas import tpu as pltpu
from jax.sharding import PartitionSpec as P

NEWTON = 2
SWEEPS = 4
OMEGA = 0.8
LANES = 128
ROWS = 8
HALO = 8
GROUPS = LANES // HALO


def params():
    return pltpu.CompilerParams(vmem_limit_bytes=48 * 2**20)


def saturation(field):
    dryness = jnp.maximum(-field, 0.0)
    return lax.rsqrt(1.0 + dryness * dryness)


def frozen_factor(freeze_state):
    return jnp.where(freeze_state == 0, 1.0, jnp.where(freeze_state == 1, 0.2, 0.02)).astype(
        jnp.float32
    )


def window_tiles(capacity):
    return capacity // LANES


def scalar_rows(count):
    return -(-count // LANES)


def to_scalars(column, staged, scalars):
    count = column.shape[0]
    for j in range(scalar_rows(count)):
        part = column[j * LANES : (j + 1) * LANES]
        shape = (part.shape[0], LANES)
        own = lax.broadcasted_iota(jnp.int32, shape, 0) == lax.broadcasted_iota(jnp.int32, shape, 1)
        staged[j : j + 1, :] = jnp.sum(jnp.where(own, part, 0), axis=0, keepdims=True)
    pltpu.sync_copy(staged, scalars)


def scalar_at(scalars, index):
    if scalars.shape[0] == 1:
        return scalars[0, index]
    return scalars[index // LANES, index % LANES]


def dispatch_kernel(layers, devices, capacity):
    chunks = window_tiles(capacity)
    fields = layers + 1
    bounds = -(-(devices + 1) // ROWS) * ROWS

    def kernel(
        block_hbm, cell_hbm, precip_hbm, evap_hbm, root_hbm, sat_hbm,
        out, starts,
        packed, block, cell, precip, evap, root, sat, staged, sems,
    ):
        columns = root.shape[1]
        copies = [
            pltpu.make_async_copy(source, target, sems.at[i])
            for i, (source, target) in enumerate(
                (
                    (block_hbm, block),
                    (root_hbm, root),
                    (sat_hbm, sat),
                    (cell_hbm, cell),
                    (precip_hbm, precip),
                    (evap_hbm, evap),
                )
            )
        ]
        for copy in copies:
            copy.start()
        copies[0].wait()
        owner_row = lax.broadcasted_iota(jnp.int32, (bounds, LANES), 0)
        before = jnp.zeros((bounds, LANES), jnp.int32)
        for r in range(columns // LANES):
            before = before + (block[r : r + 1, :] < owner_row).astype(jnp.int32)
        before = jnp.sum(before.astype(jnp.float32), axis=1, keepdims=True)
        to_scalars(before.astype(jnp.int32), staged, starts)
        for copy in copies[1:]:
            copy.wait()

        def flux(tile, carry):
            span = pl.ds(pl.multiple_of(tile * LANES, LANES), LANES)
            s = sat[:, span]
            w = root[:, span] * s * s
            total = 0.25 + jnp.sum(w, axis=0, keepdims=True)
            uptake = w * (evap[pl.ds(tile, 1), :] / total)
            top = s[0:1]
            rain = precip[pl.ds(tile, 1), :] * (1.0 - top * top * top)
            packed[0:1, span] = rain - uptake[0:1]
            packed[1:layers, span] = -uptake[1:]
            packed[layers:fields, span] = cell[pl.ds(tile, 1), :].astype(jnp.float32)
            return carry

        lax.fori_loop(0, columns // LANES, flux, 0, unroll=16)
        lane = lax.broadcasted_iota(jnp.int32, (1, LANES), 1)

        def window(owner, carry):
            start = scalar_at(starts, owner)
            count = scalar_at(starts, owner + 1) - start
            base = pl.multiple_of((start // LANES) * LANES, LANES)
            shift = start % LANES
            near = lane < LANES - shift
            turned = [
                pltpu.roll(packed[:, pl.ds(base + t * LANES, LANES)], LANES - shift, 1)
                for t in range(chunks + 1)
            ]
            for t in range(chunks):
                moved = jnp.where(near, turned[t], turned[t + 1])
                row = (owner * chunks + t) * fields
                held = t * LANES + lane < count
                out[pl.ds(row, layers), :] = moved[0:layers]
                out[pl.ds(row + layers, 1), :] = jnp.where(held, moved[layers:fields], -1.0)
            return carry

        lax.fori_loop(0, devices, window, 0, unroll=4)

    return kernel


def dispatch(block, cell, precip, evap, root, sat, devices, capacity):
    layers, columns = root.shape
    fields = layers + 1
    rows = devices * window_tiles(capacity) * fields
    bounds = scalar_rows(-(-(devices + 1) // ROWS) * ROWS)
    vmem = pl.BlockSpec(memory_space=pltpu.VMEM)
    fold = (columns // LANES, LANES)
    return pl.pallas_call(
        dispatch_kernel(layers, devices, capacity),
        out_shape=(
            jax.ShapeDtypeStruct((rows, LANES), jnp.float32),
            jax.ShapeDtypeStruct((bounds, LANES), jnp.int32),
        ),
        in_specs=[pl.BlockSpec(memory_space=pltpu.HBM)] * 6,
        out_specs=(vmem, pl.BlockSpec(memory_space=pltpu.SMEM)),
        scratch_shapes=[
            pltpu.VMEM((2 * ROWS, columns + capacity + LANES), jnp.float32),
            pltpu.VMEM(fold, jnp.int32),
            pltpu.VMEM(fold, jnp.int32),
            pltpu.VMEM(fold, jnp.float32),
            pltpu.VMEM(fold, jnp.float32),
            pltpu.VMEM(root.shape, jnp.float32),
            pltpu.VMEM(root.shape, jnp.float32),
            pltpu.VMEM((bounds, LANES), jnp.int32),
            pltpu.SemaphoreType.DMA((6,)),
        ],
        compiler_params=params(),
        name="dispatch",
    )(
        *(
            pltpu.with_memory_space_constraint(a, pltpu.HBM)
            for a in (
                block.reshape(fold),
                cell.reshape(fold),
                precip.reshape(fold),
                evap.reshape(fold),
                root,
                sat,
            )
        )
    )


def scatter_kernel(layers, cells_x, cells_y, batch):
    fields = layers + 1
    half = layers * cells_x

    def kernel(incoming, mask, out, low, high, order, total, spread, staged, used):
        chunks = incoming.shape[0] // fields
        first_cells = incoming[pl.ds(layers, chunks, stride=fields), :][:, 0:1]
        to_scalars((first_cells >= 0.0).astype(jnp.int32), staged, used)

        def listed(c, filled):
            holds = scalar_at(used, c)
            order[jnp.where(holds > 0, filled, chunks - 1 - (c - filled))] = c
            return filled + holds

        filled = lax.fori_loop(0, chunks, listed, 0, unroll=8)
        batches = (filled + batch - 1) // batch
        order[chunks] = filled
        total[...] = jnp.zeros_like(total)
        row_x = lax.broadcasted_iota(jnp.int32, (cells_x, LANES), 0)
        row_y = lax.broadcasted_iota(jnp.int32, (cells_y, LANES), 0)

        def step(i, carry):
            onehots = []
            for b in range(batch):
                first = order[i * batch + b] * fields
                cell = incoming[pl.ds(first + layers, 1), :].astype(jnp.int32)
                x = cell // cells_y
                y = cell - x * cells_y
                x = jnp.where(cell < 0, -1, x)
                onehots.append((row_y == y).astype(jnp.float32).astype(jnp.bfloat16))
                here = row_x == x
                values = incoming[pl.ds(first, layers), :]
                big = values.astype(jnp.bfloat16).astype(jnp.float32)
                small = values - big
                span = slice(b * LANES, (b + 1) * LANES)
                for k in range(layers):
                    rows = slice(k * cells_x, (k + 1) * cells_x)
                    spread[rows, span] = jnp.where(here, big[k : k + 1], 0.0).astype(jnp.bfloat16)
                    rows = slice(half + k * cells_x, half + (k + 1) * cells_x)
                    spread[rows, span] = jnp.where(here, small[k : k + 1], 0.0).astype(
                        jnp.bfloat16
                    )
            onehot = jnp.concatenate(onehots, axis=1)
            total[...] += lax.dot_general(
                spread[...],
                onehot,
                (((1,), (1,)), ((), ())),
                preferred_element_type=jnp.float32,
            )
            return carry

        lax.fori_loop(0, batches, step, 0)
        land = mask[...].astype(jnp.float32)
        for k in range(layers):
            rows = slice(k * cells_x, (k + 1) * cells_x)
            lower = slice(half + k * cells_x, half + (k + 1) * cells_x)
            source = (total[rows, :] + total[lower, :]) * land
            out[k] = source
            low[k] = source[:HALO]
            high[k] = source[cells_x - HALO :]

    return kernel


def scatter(incoming, mask, layers, cells_x, cells_y):
    chunks = incoming.shape[0] // (layers + 1)
    batch = max(b for b in (8, 6, 4, 3, 2, 1) if chunks % b == 0)
    strip = jax.ShapeDtypeStruct((layers, HALO, cells_y), jnp.float32)
    vmem = pl.BlockSpec(memory_space=pltpu.VMEM)
    return pl.pallas_call(
        scatter_kernel(layers, cells_x, cells_y, batch),
        out_shape=(
            jax.ShapeDtypeStruct((layers, cells_x, cells_y), jnp.float32),
            strip,
            strip,
            jax.ShapeDtypeStruct((chunks + 1,), jnp.int32),
        ),
        in_specs=[vmem, vmem],
        out_specs=(vmem, vmem, vmem, pl.BlockSpec(memory_space=pltpu.SMEM)),
        scratch_shapes=[
            pltpu.VMEM((2 * layers * cells_x, cells_y), jnp.float32),
            pltpu.VMEM((2 * layers * cells_x, batch * LANES), jnp.bfloat16),
            pltpu.VMEM((scalar_rows(chunks), LANES), jnp.int32),
            pltpu.SMEM((scalar_rows(chunks), LANES), jnp.int32),
        ],
        compiler_params=params(),
        name="scatter",
    )(incoming, mask)


def both_ways(low_end, high_end, axis):
    count = lax.axis_size(axis)
    forward = [(i, i + 1) for i in range(count - 1)]
    backward = [(target, source) for source, target in forward]
    return lax.ppermute(high_end, axis, forward), lax.ppermute(low_end, axis, backward)


def packed_rows(layers, cells_x):
    tiles = layers * (cells_x + 2 * HALO) // ROWS
    return -(-tiles // GROUPS) * ROWS


def tile_places(layers, cells_x):
    tiles = (cells_x + 2 * HALO) // ROWS
    for index in range(layers * tiles):
        yield index // tiles, index % tiles, index // GROUPS, index % GROUPS


def pack_kernel(layers, cells_x, cells_y):
    lane_of = lambda: lax.broadcasted_iota(jnp.int32, (ROWS, LANES), 1)

    def kernel(middle, below, above, left, right):
        fields = middle.shape[0]
        lane = lane_of()
        last = cells_x // ROWS + 1

        def column(f, k, t, cols):
            if t == 0:
                return below[f, k, :, cols]
            if t == last:
                return above[f, k, :, cols]
            return middle[f, k, (t - 1) * ROWS : t * ROWS, cols]

        for f in range(fields):
            for out, cols, offset in (
                (left, slice(0, LANES), 0),
                (right, slice(cells_y - LANES, cells_y), LANES - HALO),
            ):
                held = {}
                for k, t, place, group in tile_places(layers, cells_x):
                    tile = column(f, k, t, cols)
                    turn = (group * HALO - offset) % LANES
                    tile = pltpu.roll(tile, turn, 1) if turn else tile
                    if group == 0:
                        held[place] = tile
                    else:
                        here = (lane >= group * HALO) & (lane < (group + 1) * HALO)
                        held[place] = jnp.where(here, tile, held[place])
                for place, tile in held.items():
                    out[f, place * ROWS : (place + 1) * ROWS, :] = tile

    return kernel


def pack(middle, below, above):
    fields, layers, cells_x, cells_y = middle.shape
    out = jax.ShapeDtypeStruct((fields, packed_rows(layers, cells_x), LANES), jnp.float32)
    vmem = pl.BlockSpec(memory_space=pltpu.VMEM)
    return pl.pallas_call(
        pack_kernel(layers, cells_x, cells_y),
        out_shape=(out, out),
        in_specs=[vmem] * 3,
        out_specs=(vmem, vmem),
        compiler_params=params(),
        name="pack",
    )(middle, below, above)


def prepare_kernel(conductivity, freeze, porosity, pressure, out, low, high):
    cells_x = out.shape[2]
    perm = conductivity[...] * frozen_factor(freeze[...])
    for f, value in enumerate((perm, porosity[...], pressure[...])):
        out[f] = value
        low[f] = value[:, :HALO]
        high[f] = value[:, cells_x - HALO :]


def prepare(conductivity, freeze, porosity, pressure):
    layers, cells_x, cells_y = pressure.shape
    strip = jax.ShapeDtypeStruct((3, layers, HALO, cells_y), jnp.float32)
    vmem = pl.BlockSpec(memory_space=pltpu.VMEM)
    return pl.pallas_call(
        prepare_kernel,
        out_shape=(jax.ShapeDtypeStruct((3, layers, cells_x, cells_y), jnp.float32), strip, strip),
        in_specs=[vmem] * 4,
        out_specs=(vmem,) * 3,
        compiler_params=params(),
        name="prepare",
    )(conductivity, freeze, porosity, pressure)


def gather_slots(order, incoming, table, reply, layers, cells_x, cells_y):
    fields = layers + 1
    chunks = incoming.shape[0] // fields
    sub = lax.broadcasted_iota(jnp.int32, (ROWS, LANES), 0)
    across = cells_y // LANES
    groups = cells_x // ROWS * across

    def one(c):
        cell = incoming[pl.ds(c * fields + layers, 1), :].astype(jnp.int32)
        cell = jnp.broadcast_to(jnp.maximum(cell, 0), (ROWS, LANES))
        x = cell // cells_y
        y = cell - x * cells_y
        lane = y % LANES
        group = (x // ROWS) * across + y // LANES
        wanted = x % ROWS == sub
        rows = []
        for k in range(layers):
            value = jnp.zeros((ROWS, LANES), jnp.float32)
            for g in range(groups):
                first = HALO + g // across * ROWS
                tile = table[k, first : first + ROWS, g % across * LANES : (g % across + 1) * LANES]
                found = jnp.take_along_axis(tile, lane, axis=1, mode="promise_in_bounds")
                value = jnp.where(group == g, found, value)
            value = jnp.where(wanted, value, 0.0)
            rows.append(jnp.sum(value, axis=0, keepdims=True))
        reply[pl.ds(c * layers, layers), :] = jnp.concatenate(rows, axis=0)

    together = max(b for b in (4, 3, 2, 1) if chunks % b == 0)

    def body(i, carry):
        for b in range(together):
            one(order[i * together + b])
        return carry

    lax.fori_loop(0, (order[chunks] + together - 1) // together, body, 0)


def newton_kernel(layers, cells_x, cells_y):
    high_x = cells_x + 2 * HALO
    wide = cells_y + LANES

    def up(v):
        return pltpu.roll(v, high_x - 1, 0)

    def down(v):
        return pltpu.roll(v, 1, 0)

    def right(v):
        return pltpu.roll(v, wide - 1, 1)

    def left(v):
        return pltpu.roll(v, 1, 1)

    def each_layer(do):
        for k in range(layers):
            do(k)

    def kernel(
        fixed, fixed_low, fixed_high, fixed_left, fixed_right,
        src, src_low, src_high, src_left, src_right, incoming, order,
        new_pressure, reply,
        perm, poro, source, pres, stored,
        tx, ty, tz, rel, gz, flow,
        ax, bx, ay, by, az, bz, resid, update,
    ):
        lane = lax.broadcasted_iota(jnp.int32, (ROWS, LANES), 1)
        last = cells_x // ROWS + 1

        def widen(dest, field, middle, low, high, side_left, side_right):
            dest[:, HALO : HALO + cells_x, :cells_y] = middle[field]
            dest[:, :HALO, :cells_y] = low[field]
            dest[:, HALO + cells_x :, :cells_y] = high[field]
            for k, t, place, group in tile_places(layers, cells_x):
                rows = slice(place * ROWS, (place + 1) * ROWS)
                turn = (LANES - HALO - group * HALO) % LANES
                a = side_left[field, rows, :]
                a = pltpu.roll(a, turn, 1) if turn else a
                turn = (-group * HALO) % LANES
                b = side_right[field, rows, :]
                b = pltpu.roll(b, turn, 1) if turn else b
                tile = jnp.where(lane < HALO, b, jnp.where(lane >= LANES - HALO, a, 0.0))
                dest[k, t * ROWS : (t + 1) * ROWS, cells_y:] = tile

        widen(perm, 0, fixed, fixed_low, fixed_high, fixed_left, fixed_right)
        widen(poro, 1, fixed, fixed_low, fixed_high, fixed_left, fixed_right)
        widen(pres, 2, fixed, fixed_low, fixed_high, fixed_left, fixed_right)
        widen(source, 0, src, src_low, src_high, src_left, src_right)

        def face(a, b):
            joined = a + b
            return a * b / jnp.where(joined > 0.0, joined, 1.0)

        def still(k):
            a = perm[k]
            tx[k] = face(a, up(a))
            ty[k] = face(a, right(a))
            tz[k] = face(a, perm[min(k + 1, layers - 1)])
            stored[k] = saturation(pres[k])

        each_layer(still)

        for newton_step in range(NEWTON):

            def relative(k):
                s = saturation(pres[k])
                rel[k] = s * s * s

            each_layer(relative)

            def vertical(k):
                r = rel[k]
                below = min(k + 1, layers - 1)
                g = tz[k] * (r + rel[below])
                if k < layers - 1:
                    gz[k + 1] = g
                    flow[k + 1] = g * (pres[k] - pres[below] + 1.0)
                else:
                    gz[k + 1] = jnp.zeros_like(g)
                    flow[k + 1] = perm[k] * r

            gz[0] = jnp.zeros((high_x, wide), jnp.float32)
            flow[0] = jnp.zeros((high_x, wide), jnp.float32)
            each_layer(vertical)

            def linear(k):
                p = pres[k]
                r = rel[k]
                gx = tx[k] * (r + up(r))
                gy = ty[k] * (r + right(r))
                fx = gx * (p - up(p))
                fy = gy * (p - right(p))
                gxd = down(gx)
                gyd = left(gy)
                s = saturation(p)
                porous = poro[k]
                residual = porous * (s - stored[k])
                residual = residual + (fx - down(fx)) + (fy - left(fy))
                residual = residual + (flow[k + 1] - flow[k]) - source[k]
                gzd = gz[k]
                gzu = gz[k + 1]
                diagonal = porous * (jnp.maximum(-p, 0.0) * r)
                diagonal = diagonal + (gx + gxd) + (gy + gyd) + (gzu + gzd)
                diagonal = jnp.where(diagonal > 0.0, diagonal, 1.0)
                scale = OMEGA / diagonal
                ax[k] = scale * gx
                bx[k] = scale * gxd
                ay[k] = scale * gy
                by[k] = scale * gyd
                az[k] = scale * gzu
                bz[k] = scale * gzd
                residual = scale * residual
                resid[k] = residual
                update[0, k] = -residual

            each_layer(linear)

            for sweep in range(SWEEPS - 1):
                old = sweep % 2
                new = 1 - old

                def smooth(k):
                    u = update[old, k]
                    v = (1.0 - OMEGA) * u - resid[k]
                    v = v + ax[k] * up(u) + bx[k] * down(u)
                    v = v + ay[k] * right(u) + by[k] * left(u)
                    v = v + az[k] * update[old, min(k + 1, layers - 1)]
                    v = v + bz[k] * update[old, max(k - 1, 0)]
                    update[new, k] = v
                    if sweep == SWEEPS - 2:
                        pres[k] = pres[k] + v

                each_layer(smooth)

        def finish(k):
            p = pres[k, HALO : HALO + cells_x, :cells_y]
            new_pressure[k] = p
            rel[k, HALO : HALO + cells_x, :cells_y] = saturation(p)

        each_layer(finish)
        gather_slots(order, incoming, rel, reply, layers, cells_x, cells_y)

    return kernel


def newton(fixed, source, incoming, order, layers, cells_x, cells_y):
    chunks = incoming.shape[0] // (layers + 1)
    high_x, wide = cells_x + 2 * HALO, cells_y + LANES
    field = pltpu.VMEM((layers, high_x, wide), jnp.float32)
    taller = pltpu.VMEM((layers + 1, high_x, wide), jnp.float32)
    vmem = pl.BlockSpec(memory_space=pltpu.VMEM)
    return pl.pallas_call(
        newton_kernel(layers, cells_x, cells_y),
        out_shape=(
            jax.ShapeDtypeStruct((layers, cells_x, cells_y), jnp.float32),
            jax.ShapeDtypeStruct((chunks * layers, LANES), jnp.float32),
        ),
        in_specs=[vmem] * 11 + [pl.BlockSpec(memory_space=pltpu.SMEM)],
        out_specs=(vmem, vmem),
        scratch_shapes=[field] * 5
        + [field] * 4
        + [taller] * 2
        + [field] * 7
        + [pltpu.VMEM((2, layers, high_x, wide), jnp.float32)],
        compiler_params=params(),
        name="newton",
    )(*fixed, *source, incoming, order)


def combine_kernel(layers, devices, capacity):
    chunks = window_tiles(capacity)

    def kernel(starts, answer, out, wide):
        lane = lax.broadcasted_iota(jnp.int32, (1, LANES), 1)

        def window(owner, carry):
            start = scalar_at(starts, owner)
            base = pl.multiple_of((start // LANES) * LANES, LANES)
            shift = start % LANES
            before = lane < shift
            row = owner * chunks * layers
            kept = wide[0:layers, pl.ds(base, LANES)]
            for t in range(chunks):
                turned = pltpu.roll(answer[pl.ds(row + t * layers, layers), :], shift, 1)
                wide[0:layers, pl.ds(base + t * LANES, LANES)] = jnp.where(before, kept, turned)
                kept = turned
            wide[0:layers, pl.ds(base + chunks * LANES, LANES)] = kept
            return carry

        lax.fori_loop(0, devices, window, 0, unroll=4)
        out[...] = wide[0:layers, : out.shape[1]]

    return kernel


def combine(starts, answer, layers, columns, devices, capacity):
    vmem = pl.BlockSpec(memory_space=pltpu.VMEM)
    return pl.pallas_call(
        combine_kernel(layers, devices, capacity),
        out_shape=jax.ShapeDtypeStruct((layers, columns), jnp.float32),
        in_specs=[pl.BlockSpec(memory_space=pltpu.SMEM), vmem],
        out_specs=vmem,
        scratch_shapes=[pltpu.VMEM((2 * ROWS, columns + capacity + LANES), jnp.float32)],
        compiler_params=params(),
        name="combine",
    )(starts, answer)


def on_device(
    clm_block,
    clm_cell,
    precip,
    evap_demand,
    root_share,
    sat_before,
    pressure,
    conductivity,
    porosity,
    freeze_state,
    land_mask,
):
    axes = ("gx", "gy")
    layers, columns = root_share.shape
    devices = lax.axis_size("gx") * lax.axis_size("gy")
    cells_x, cells_y = pressure.shape[1], pressure.shape[2]
    per_pair = columns // devices
    capacity = -(-(per_pair + per_pair // 2) // LANES) * LANES
    outgoing, starts = dispatch(
        clm_block, clm_cell, precip, evap_demand, root_share, sat_before, devices, capacity
    )
    flat = lax.all_to_all(outgoing.reshape(-1), axes, split_axis=0, concat_axis=0, tiled=True)
    incoming = flat.reshape(outgoing.shape)

    fixed, low, high = prepare(conductivity, freeze_state, porosity, pressure)
    below, above = both_ways(low, high, "gx")
    to_left, to_right = pack(fixed, below, above)
    side_left, side_right = both_ways(to_left, to_right, "gy")
    fixed = (fixed, below, above, side_left, side_right)

    source, low, high, order = scatter(incoming, land_mask, layers, cells_x, cells_y)
    below, above = both_ways(low, high, "gx")
    source, below, above = source[None], below[None], above[None]
    to_left, to_right = pack(source, below, above)
    side_left, side_right = both_ways(to_left, to_right, "gy")
    source = (source, below, above, side_left, side_right)

    new_pressure, reply = newton(fixed, source, incoming, order, layers, cells_x, cells_y)
    flat = lax.all_to_all(reply.reshape(-1), axes, split_axis=0, concat_axis=0, tiled=True)
    returned = combine(starts, flat.reshape(reply.shape), layers, columns, devices, capacity)
    return (new_pressure, returned)


def solution(mesh):
    columns = P(("gx", "gy"))
    layered = P(None, ("gx", "gy"))
    grid = P(None, "gx", "gy")
    return jax.shard_map(
        on_device,
        mesh=mesh,
        in_specs=(columns,) * 4 + (layered,) * 2 + (grid,) * 4 + (P("gx", "gy"),),
        out_specs=(grid, layered),
        check_vma=False,
    )
```

```python
import jax
import jax.numpy as jnp
from jax import lax
from jax.experimental import pallas as pl
from jax.experimental.pallas import tpu as pltpu
from jax.sharding import PartitionSpec as P

NEWTON = 2
SWEEPS = 4
OMEGA = 0.8
LANES = 128
ROWS = 8
HALO = 8
GROUPS = LANES // HALO


def params(mebibytes=16):
    return pltpu.CompilerParams(vmem_limit_bytes=mebibytes * 2**20)


def saturation(field):
    dryness = jnp.maximum(-field, 0.0)
    return lax.rsqrt(1.0 + dryness * dryness)


def frozen_factor(freeze_state):
    return jnp.where(freeze_state == 0, 1.0, jnp.where(freeze_state == 1, 0.2, 0.02)).astype(
        jnp.float32
    )


def window_tiles(capacity):
    return capacity // LANES


def scalar_rows(count):
    return -(-count // LANES)


def to_scalars(column, staged, scalars):
    count = column.shape[0]
    for j in range(scalar_rows(count)):
        part = column[j * LANES : (j + 1) * LANES]
        shape = (part.shape[0], LANES)
        own = lax.broadcasted_iota(jnp.int32, shape, 0) == lax.broadcasted_iota(jnp.int32, shape, 1)
        staged[j : j + 1, :] = jnp.sum(jnp.where(own, part, 0), axis=0, keepdims=True)
    pltpu.sync_copy(staged, scalars)


def scalar_at(scalars, index):
    if scalars.shape[0] == 1:
        return scalars[0, index]
    return scalars[index // LANES, index % LANES]


def dispatch_kernel(layers, devices, capacity):
    chunks = window_tiles(capacity)
    fields = layers + 1
    bounds = -(-(devices + 1) // ROWS) * ROWS

    def kernel(
        block_hbm, cell_hbm, precip_hbm, evap_hbm, root_hbm, sat_hbm,
        out, starts,
        packed, block, cell, precip, evap, root, sat, staged, sems,
    ):
        columns = root.shape[1]
        copies = [
            pltpu.make_async_copy(source, target, sems.at[i])
            for i, (source, target) in enumerate(
                (
                    (block_hbm, block),
                    (root_hbm, root),
                    (sat_hbm, sat),
                    (cell_hbm, cell),
                    (precip_hbm, precip),
                    (evap_hbm, evap),
                )
            )
        ]
        for copy in copies:
            copy.start()
        copies[0].wait()
        owner_row = lax.broadcasted_iota(jnp.int32, (bounds, LANES), 0)
        before = jnp.zeros((bounds, LANES), jnp.int32)
        for r in range(columns // LANES):
            before = before + (block[r : r + 1, :] < owner_row).astype(jnp.int32)
        before = jnp.sum(before.astype(jnp.float32), axis=1, keepdims=True)
        to_scalars(before.astype(jnp.int32), staged, starts)
        for copy in copies[1:]:
            copy.wait()

        def flux(tile, carry):
            span = pl.ds(pl.multiple_of(tile * LANES, LANES), LANES)
            s = sat[:, span]
            w = root[:, span] * s * s
            total = 0.25 + jnp.sum(w, axis=0, keepdims=True)
            uptake = w * (evap[pl.ds(tile, 1), :] / total)
            top = s[0:1]
            rain = precip[pl.ds(tile, 1), :] * (1.0 - top * top * top)
            packed[0:1, span] = rain - uptake[0:1]
            packed[1:layers, span] = -uptake[1:]
            packed[layers:fields, span] = cell[pl.ds(tile, 1), :].astype(jnp.float32)
            return carry

        lax.fori_loop(0, columns // LANES, flux, 0, unroll=16)
        lane = lax.broadcasted_iota(jnp.int32, (1, LANES), 1)

        def window(owner, carry):
            start = scalar_at(starts, owner)
            count = scalar_at(starts, owner + 1) - start
            base = pl.multiple_of((start // LANES) * LANES, LANES)
            shift = start % LANES
            near = lane < LANES - shift
            turned = [
                pltpu.roll(packed[:, pl.ds(base + t * LANES, LANES)], LANES - shift, 1)
                for t in range(chunks + 1)
            ]
            for t in range(chunks):
                moved = jnp.where(near, turned[t], turned[t + 1])
                row = (owner * chunks + t) * fields
                held = t * LANES + lane < count
                out[pl.ds(row, layers), :] = moved[0:layers]
                out[pl.ds(row + layers, 1), :] = jnp.where(held, moved[layers:fields], -1.0)
            return carry

        lax.fori_loop(0, devices, window, 0, unroll=4)

    return kernel


def dispatch(block, cell, precip, evap, root, sat, devices, capacity):
    layers, columns = root.shape
    fields = layers + 1
    rows = devices * window_tiles(capacity) * fields
    bounds = scalar_rows(-(-(devices + 1) // ROWS) * ROWS)
    vmem = pl.BlockSpec(memory_space=pltpu.VMEM)
    fold = (columns // LANES, LANES)
    return pl.pallas_call(
        dispatch_kernel(layers, devices, capacity),
        out_shape=(
            jax.ShapeDtypeStruct((rows, LANES), jnp.float32),
            jax.ShapeDtypeStruct((bounds, LANES), jnp.int32),
        ),
        in_specs=[pl.BlockSpec(memory_space=pltpu.HBM)] * 6,
        out_specs=(vmem, pl.BlockSpec(memory_space=pltpu.SMEM)),
        scratch_shapes=[
            pltpu.VMEM((2 * ROWS, columns + capacity + LANES), jnp.float32),
            pltpu.VMEM(fold, jnp.int32),
            pltpu.VMEM(fold, jnp.int32),
            pltpu.VMEM(fold, jnp.float32),
            pltpu.VMEM(fold, jnp.float32),
            pltpu.VMEM(root.shape, jnp.float32),
            pltpu.VMEM(root.shape, jnp.float32),
            pltpu.VMEM((bounds, LANES), jnp.int32),
            pltpu.SemaphoreType.DMA((6,)),
        ],
        compiler_params=params(),
        name="dispatch",
    )(
        *(
            pltpu.with_memory_space_constraint(a, pltpu.HBM)
            for a in (
                block.reshape(fold),
                cell.reshape(fold),
                precip.reshape(fold),
                evap.reshape(fold),
                root,
                sat,
            )
        )
    )


def scatter_kernel(layers, cells_x, cells_y, batch):
    fields = layers + 1
    half = layers * cells_x

    def kernel(incoming, mask, out, low, high, order, total, spread, staged, used):
        chunks = incoming.shape[0] // fields
        first_cells = incoming[pl.ds(layers, chunks, stride=fields), :][:, 0:1]
        to_scalars((first_cells >= 0.0).astype(jnp.int32), staged, used)

        def listed(c, filled):
            holds = scalar_at(used, c)
            order[jnp.where(holds > 0, filled, chunks - 1 - (c - filled))] = c
            return filled + holds

        filled = lax.fori_loop(0, chunks, listed, 0, unroll=8)
        batches = (filled + batch - 1) // batch
        order[chunks] = filled
        total[...] = jnp.zeros_like(total)
        row_x = lax.broadcasted_iota(jnp.int32, (cells_x, LANES), 0)
        row_y = lax.broadcasted_iota(jnp.int32, (cells_y, LANES), 0)

        def step(i, carry):
            onehots = []
            for b in range(batch):
                first = order[i * batch + b] * fields
                cell = incoming[pl.ds(first + layers, 1), :].astype(jnp.int32)
                x = cell // cells_y
                y = cell - x * cells_y
                x = jnp.where(cell < 0, -1, x)
                onehots.append((row_y == y).astype(jnp.float32).astype(jnp.bfloat16))
                here = row_x == x
                values = incoming[pl.ds(first, layers), :]
                big = values.astype(jnp.bfloat16).astype(jnp.float32)
                small = values - big
                span = slice(b * LANES, (b + 1) * LANES)
                for k in range(layers):
                    rows = slice(k * cells_x, (k + 1) * cells_x)
                    spread[rows, span] = jnp.where(here, big[k : k + 1], 0.0).astype(jnp.bfloat16)
                    rows = slice(half + k * cells_x, half + (k + 1) * cells_x)
                    spread[rows, span] = jnp.where(here, small[k : k + 1], 0.0).astype(
                        jnp.bfloat16
                    )
            onehot = jnp.concatenate(onehots, axis=1)
            total[...] += lax.dot_general(
                spread[...],
                onehot,
                (((1,), (1,)), ((), ())),
                preferred_element_type=jnp.float32,
            )
            return carry

        lax.fori_loop(0, batches, step, 0)
        land = mask[...].astype(jnp.float32)
        for k in range(layers):
            rows = slice(k * cells_x, (k + 1) * cells_x)
            lower = slice(half + k * cells_x, half + (k + 1) * cells_x)
            source = (total[rows, :] + total[lower, :]) * land
            out[k] = source
            low[k] = source[:HALO]
            high[k] = source[cells_x - HALO :]

    return kernel


def scatter(incoming, mask, layers, cells_x, cells_y):
    chunks = incoming.shape[0] // (layers + 1)
    batch = max(b for b in (8, 6, 4, 3, 2, 1) if chunks % b == 0)
    strip = jax.ShapeDtypeStruct((layers, HALO, cells_y), jnp.float32)
    vmem = pl.BlockSpec(memory_space=pltpu.VMEM)
    return pl.pallas_call(
        scatter_kernel(layers, cells_x, cells_y, batch),
        out_shape=(
            jax.ShapeDtypeStruct((layers, cells_x, cells_y), jnp.float32),
            strip,
            strip,
            jax.ShapeDtypeStruct((chunks + 1,), jnp.int32),
        ),
        in_specs=[vmem, vmem],
        out_specs=(vmem, vmem, vmem, pl.BlockSpec(memory_space=pltpu.SMEM)),
        scratch_shapes=[
            pltpu.VMEM((2 * layers * cells_x, cells_y), jnp.float32),
            pltpu.VMEM((2 * layers * cells_x, batch * LANES), jnp.bfloat16),
            pltpu.VMEM((scalar_rows(chunks), LANES), jnp.int32),
            pltpu.SMEM((scalar_rows(chunks), LANES), jnp.int32),
        ],
        compiler_params=params(),
        name="scatter",
    )(incoming, mask)


def both_ways(low_end, high_end, axis):
    count = lax.axis_size(axis)
    forward = [(i, i + 1) for i in range(count - 1)]
    backward = [(target, source) for source, target in forward]
    return lax.ppermute(high_end, axis, forward), lax.ppermute(low_end, axis, backward)


def packed_rows(layers, cells_x):
    tiles = layers * (cells_x + 2 * HALO) // ROWS
    return -(-tiles // GROUPS) * ROWS


def tile_places(layers, cells_x):
    tiles = (cells_x + 2 * HALO) // ROWS
    for index in range(layers * tiles):
        yield index // tiles, index % tiles, index // GROUPS, index % GROUPS


def pack_kernel(layers, cells_x, cells_y):
    lane_of = lambda: lax.broadcasted_iota(jnp.int32, (ROWS, LANES), 1)

    def kernel(middle, below, above, left, right):
        fields = middle.shape[0]
        lane = lane_of()
        last = cells_x // ROWS + 1

        def column(f, k, t, cols):
            if t == 0:
                return below[f, k, :, cols]
            if t == last:
                return above[f, k, :, cols]
            return middle[f, k, (t - 1) * ROWS : t * ROWS, cols]

        for f in range(fields):
            for out, cols, offset in (
                (left, slice(0, LANES), 0),
                (right, slice(cells_y - LANES, cells_y), LANES - HALO),
            ):
                held = {}
                for k, t, place, group in tile_places(layers, cells_x):
                    tile = column(f, k, t, cols)
                    turn = (group * HALO - offset) % LANES
                    tile = pltpu.roll(tile, turn, 1) if turn else tile
                    if group == 0:
                        held[place] = tile
                    else:
                        here = (lane >= group * HALO) & (lane < (group + 1) * HALO)
                        held[place] = jnp.where(here, tile, held[place])
                for place, tile in held.items():
                    out[f, place * ROWS : (place + 1) * ROWS, :] = tile

    return kernel


def pack(middle, below, above):
    fields, layers, cells_x, cells_y = middle.shape
    out = jax.ShapeDtypeStruct((fields, packed_rows(layers, cells_x), LANES), jnp.float32)
    vmem = pl.BlockSpec(memory_space=pltpu.VMEM)
    return pl.pallas_call(
        pack_kernel(layers, cells_x, cells_y),
        out_shape=(out, out),
        in_specs=[vmem] * 3,
        out_specs=(vmem, vmem),
        compiler_params=params(),
        name="pack",
    )(middle, below, above)


def prepare_kernel(conductivity, freeze, porosity, pressure, out, low, high):
    cells_x = out.shape[2]
    perm = conductivity[...] * frozen_factor(freeze[...])
    for f, value in enumerate((perm, porosity[...], pressure[...])):
        out[f] = value
        low[f] = value[:, :HALO]
        high[f] = value[:, cells_x - HALO :]


def prepare(conductivity, freeze, porosity, pressure):
    layers, cells_x, cells_y = pressure.shape
    strip = jax.ShapeDtypeStruct((3, layers, HALO, cells_y), jnp.float32)
    vmem = pl.BlockSpec(memory_space=pltpu.VMEM)
    return pl.pallas_call(
        prepare_kernel,
        out_shape=(jax.ShapeDtypeStruct((3, layers, cells_x, cells_y), jnp.float32), strip, strip),
        in_specs=[vmem] * 4,
        out_specs=(vmem,) * 3,
        compiler_params=params(),
        name="prepare",
    )(conductivity, freeze, porosity, pressure)


def gather_slots(order, incoming, table, split, reply, layers, cells_x, cells_y, turned):
    fields = layers + 1
    chunks = incoming.shape[0] // fields
    sub = lax.broadcasted_iota(jnp.int32, (ROWS, LANES), 0)
    row_x = lax.broadcasted_iota(jnp.int32, (cells_x, LANES), 0)
    row_y = lax.broadcasted_iota(jnp.int32, (cells_y, LANES), 0)
    across = cells_y // LANES
    groups = cells_x // ROWS * across
    half = split.shape[0] // 2
    together = max(b for b in (8, 4, 3, 2, 1) if chunks % b == 0)

    def looked_up(cell):
        cell = jnp.broadcast_to(cell, (ROWS, LANES))
        x = cell // cells_y
        y = cell - x * cells_y
        lane = y % LANES
        group = (x // ROWS) * across + y // LANES
        wanted = x % ROWS == sub
        rows = []
        for k in range(turned):
            value = jnp.zeros((ROWS, LANES), jnp.float32)
            for g in range(groups):
                first = HALO + g // across * ROWS
                tile = table[k, first : first + ROWS, g % across * LANES : (g % across + 1) * LANES]
                found = jnp.take_along_axis(tile, lane, axis=1, mode="promise_in_bounds")
                value = jnp.where(group == g, found, value)
            value = jnp.where(wanted, value, 0.0)
            rows.append(jnp.sum(value, axis=0, keepdims=True))
        return rows

    def body(i, carry):
        places = [order[i * together + b] for b in range(together)]
        cells = []
        onehots = []
        for c in places:
            cell = jnp.maximum(incoming[pl.ds(c * fields + layers, 1), :].astype(jnp.int32), 0)
            cells.append(cell)
            onehots.append((row_y == cell % cells_y).astype(jnp.float32).astype(jnp.bfloat16))
        product = jnp.dot(
            split[...], jnp.concatenate(onehots, axis=1), preferred_element_type=jnp.float32
        )
        for b, c in enumerate(places):
            rows = looked_up(cells[b])
            here = row_x == cells[b] // cells_y
            span = slice(b * LANES, (b + 1) * LANES)
            for k in range(layers - turned):
                upper = product[k * cells_x : (k + 1) * cells_x, span]
                lower = product[half + k * cells_x : half + (k + 1) * cells_x, span]
                found = jnp.where(here, upper + lower, 0.0)
                rows.append(jnp.sum(found, axis=0, keepdims=True))
            reply[pl.ds(c * layers, layers), :] = jnp.concatenate(rows, axis=0)
        return carry

    lax.fori_loop(0, (order[chunks] + together - 1) // together, body, 0)


class Stencil:
    def __init__(self, layers, cells_x, cells_y):
        self.layers, self.cells_x, self.cells_y = layers, cells_x, cells_y
        self.high_x, self.wide = cells_x + 2 * HALO, cells_y + LANES

    def up(self, v):
        return pltpu.roll(v, self.high_x - 1, 0)

    def down(self, v):
        return pltpu.roll(v, 1, 0)

    def right(self, v):
        return pltpu.roll(v, self.wide - 1, 1)

    def left(self, v):
        return pltpu.roll(v, 1, 1)

    def each_layer(self, do):
        for k in range(self.layers):
            do(k)

    def widen(self, dest, field, middle, low, high, side_left, side_right):
        layers, cells_x, cells_y = self.layers, self.cells_x, self.cells_y
        lane = lax.broadcasted_iota(jnp.int32, (ROWS, LANES), 1)
        dest[:, HALO : HALO + cells_x, :cells_y] = middle[field]
        dest[:, :HALO, :cells_y] = low[field]
        dest[:, HALO + cells_x :, :cells_y] = high[field]
        for k, t, place, group in tile_places(layers, cells_x):
            rows = slice(place * ROWS, (place + 1) * ROWS)
            turn = (LANES - HALO - group * HALO) % LANES
            a = side_left[field, rows, :]
            a = pltpu.roll(a, turn, 1) if turn else a
            turn = (-group * HALO) % LANES
            b = side_right[field, rows, :]
            b = pltpu.roll(b, turn, 1) if turn else b
            tile = jnp.where(lane < HALO, b, jnp.where(lane >= LANES - HALO, a, 0.0))
            dest[k, t * ROWS : (t + 1) * ROWS, cells_y:] = tile

    def faces(self, perm, tx, ty, tz):
        def face(a, b):
            joined = a + b
            return a * b / jnp.where(joined > 0.0, joined, 1.0)

        def still(k):
            a = perm[k]
            tx[k] = face(a, self.up(a))
            ty[k] = face(a, self.right(a))
            tz[k] = face(a, perm[min(k + 1, self.layers - 1)])

        self.each_layer(still)

    def linearize(self, pres, poro, stored, last_perm, tx, ty, tz, rel, gz, flow, weights, finish):
        ax, bx, ay, by, az, bz = weights
        layers = self.layers

        def relative(k):
            s = saturation(pres[k])
            rel[k] = s * s * s

        self.each_layer(relative)
        nothing = jnp.zeros((self.high_x, self.wide), jnp.float32)
        gz[0] = nothing
        flow[0] = nothing

        def vertical(k):
            r = rel[k]
            if k < layers - 1:
                g = tz[k] * (r + rel[k + 1])
                gz[k + 1] = g
                flow[k + 1] = g * (pres[k] - pres[k + 1] + 1.0)
            else:
                gz[k + 1] = nothing
                flow[k + 1] = last_perm * r

        self.each_layer(vertical)

        def linear(k):
            p = pres[k]
            r = rel[k]
            gx = tx[k] * (r + self.up(r))
            gy = ty[k] * (r + self.right(r))
            fx = gx * (p - self.up(p))
            fy = gy * (p - self.right(p))
            gxd = self.down(gx)
            gyd = self.left(gy)
            s = saturation(p)
            porous = poro[k]
            residual = porous * (s - stored[k])
            residual = residual + (fx - self.down(fx)) + (fy - self.left(fy))
            residual = residual + (flow[k + 1] - flow[k])
            gzd = gz[k]
            gzu = gz[k + 1]
            diagonal = porous * (jnp.maximum(-p, 0.0) * r)
            diagonal = diagonal + (gx + gxd) + (gy + gyd) + (gzu + gzd)
            diagonal = jnp.where(diagonal > 0.0, diagonal, 1.0)
            scale = OMEGA / diagonal
            ax[k] = scale * gx
            bx[k] = scale * gxd
            ay[k] = scale * gy
            by[k] = scale * gyd
            az[k] = scale * gzu
            bz[k] = scale * gzd
            finish(k, residual, scale)

        self.each_layer(linear)

    def sweeps(self, pres, weights, resid, update):
        ax, bx, ay, by, az, bz = weights
        layers = self.layers
        for sweep in range(SWEEPS - 1):
            old = sweep % 2
            new = 1 - old

            def smooth(k):
                u = update[old, k]
                v = (1.0 - OMEGA) * u - resid[k]
                v = v + ax[k] * self.up(u) + bx[k] * self.down(u)
                v = v + ay[k] * self.right(u) + by[k] * self.left(u)
                v = v + az[k] * update[old, min(k + 1, layers - 1)]
                v = v + bz[k] * update[old, max(k - 1, 0)]
                update[new, k] = v
                if sweep == SWEEPS - 2:
                    pres[k] = pres[k] + v

            self.each_layer(smooth)


def begin_kernel(grid):
    def kernel(
        fixed, low, high, side_left, side_right,
        pres, poro, stored, last_perm, tx, ty, tz, ax, bx, ay, by, az, bz, resid, scales,
        perm, rel, gz, flow,
    ):
        sides = (low, high, side_left, side_right)
        grid.widen(perm, 0, fixed, *sides)
        grid.widen(poro, 1, fixed, *sides)
        grid.widen(pres, 2, fixed, *sides)
        grid.faces(perm, tx, ty, tz)
        last_perm[...] = perm[grid.layers - 1]

        def keep(k):
            stored[k] = saturation(pres[k])

        grid.each_layer(keep)

        def finish(k, residual, scale):
            resid[k] = scale * residual
            scales[k] = scale

        grid.linearize(
            pres, poro, stored, last_perm[...], tx, ty, tz, rel, gz, flow,
            (ax, bx, ay, by, az, bz), finish,
        )

    return kernel


def begin(fixed, layers, cells_x, cells_y):
    grid = Stencil(layers, cells_x, cells_y)
    shape = (layers, grid.high_x, grid.wide)
    field = jax.ShapeDtypeStruct(shape, jnp.float32)
    plane = jax.ShapeDtypeStruct(shape[1:], jnp.float32)
    vmem = pl.BlockSpec(memory_space=pltpu.VMEM)
    outs = (field,) * 3 + (plane,) + (field,) * 11
    cells = layers * grid.high_x * grid.wide
    return pl.pallas_call(
        begin_kernel(grid),
        out_shape=outs,
        in_specs=[vmem] * 5,
        out_specs=(vmem,) * len(outs),
        scratch_shapes=[pltpu.VMEM(shape, jnp.float32)] * 2
        + [pltpu.VMEM((layers + 1,) + shape[1:], jnp.float32)] * 2,
        compiler_params=params(24),
        cost_estimate=pl.CostEstimate(
            flops=100 * cells, transcendentals=4 * cells, bytes_accessed=0
        ),
        name="begin",
    )(*fixed)


def newton_kernel(grid, turned):
    layers, cells_x, cells_y = grid.layers, grid.cells_x, grid.cells_y

    def kernel(
        pres0, poro, stored, last_perm, tx, ty, tz,
        ax0, bx0, ay0, by0, az0, bz0, resid0, scales,
        src, src_low, src_high, src_left, src_right, incoming, order,
        new_pressure, reply,
        source, pres, rel, gz, flow, ax, bx, ay, by, az, bz, resid, update, split,
    ):
        grid.widen(source, 0, src, src_low, src_high, src_left, src_right)

        def first(k):
            pres[k] = pres0[k]
            residual = resid0[k] - scales[k] * source[k]
            resid[k] = residual
            update[0, k] = -residual

        grid.each_layer(first)
        grid.sweeps(pres, (ax0, bx0, ay0, by0, az0, bz0), resid, update)
        weights = (ax, bx, ay, by, az, bz)
        for newton_step in range(1, NEWTON):

            def finish(k, residual, scale):
                residual = scale * (residual - source[k])
                resid[k] = residual
                update[0, k] = -residual

            grid.linearize(
                pres, poro, stored, last_perm[...], tx, ty, tz, rel, gz, flow, weights, finish
            )
            grid.sweeps(pres, weights, resid, update)

        half = split.shape[0] // 2
        for k in range(layers):
            p = pres[k, HALO : HALO + cells_x, :cells_y]
            new_pressure[k] = p
            s = saturation(p)
            if k < turned:
                rel[k, HALO : HALO + cells_x, :cells_y] = s
            else:
                row = (k - turned) * cells_x
                upper = s.astype(jnp.bfloat16)
                split[row : row + cells_x, :] = upper
                lower = (s - upper.astype(jnp.float32)).astype(jnp.bfloat16)
                split[half + row : half + row + cells_x, :] = lower
        gather_slots(order, incoming, rel, split, reply, layers, cells_x, cells_y, turned)

    return kernel


def newton(begun, source, incoming, order, layers, cells_x, cells_y):
    grid = Stencil(layers, cells_x, cells_y)
    turned = 5
    chunks = incoming.shape[0] // (layers + 1)
    shape = (layers, grid.high_x, grid.wide)
    field = pltpu.VMEM(shape, jnp.float32)
    taller = pltpu.VMEM((layers + 1,) + shape[1:], jnp.float32)
    vmem = pl.BlockSpec(memory_space=pltpu.VMEM)
    return pl.pallas_call(
        newton_kernel(grid, turned),
        out_shape=(
            jax.ShapeDtypeStruct((layers, cells_x, cells_y), jnp.float32),
            jax.ShapeDtypeStruct((chunks * layers, LANES), jnp.float32),
        ),
        in_specs=[vmem] * 21 + [pl.BlockSpec(memory_space=pltpu.SMEM)],
        out_specs=(vmem, vmem),
        scratch_shapes=[field] * 3
        + [taller] * 2
        + [field] * 7
        + [
            pltpu.VMEM((2,) + shape, jnp.float32),
            pltpu.VMEM((2 * (layers - turned) * cells_x, cells_y), jnp.bfloat16),
        ],
        compiler_params=params(32),
        name="newton",
    )(*begun, *source, incoming, order)


def combine_kernel(layers, devices, capacity):
    chunks = window_tiles(capacity)

    def kernel(starts, answer, out, wide):
        lane = lax.broadcasted_iota(jnp.int32, (1, LANES), 1)

        def window(owner, carry):
            start = scalar_at(starts, owner)
            base = pl.multiple_of((start // LANES) * LANES, LANES)
            shift = start % LANES
            before = lane < shift
            row = owner * chunks * layers
            kept = wide[0:layers, pl.ds(base, LANES)]
            for t in range(chunks):
                turned = pltpu.roll(answer[pl.ds(row + t * layers, layers), :], shift, 1)
                wide[0:layers, pl.ds(base + t * LANES, LANES)] = jnp.where(before, kept, turned)
                kept = turned
            wide[0:layers, pl.ds(base + chunks * LANES, LANES)] = kept
            return carry

        lax.fori_loop(0, devices, window, 0, unroll=4)
        out[...] = wide[0:layers, : out.shape[1]]

    return kernel


def combine(starts, answer, layers, columns, devices, capacity):
    vmem = pl.BlockSpec(memory_space=pltpu.VMEM)
    return pl.pallas_call(
        combine_kernel(layers, devices, capacity),
        out_shape=jax.ShapeDtypeStruct((layers, columns), jnp.float32),
        in_specs=[pl.BlockSpec(memory_space=pltpu.SMEM), vmem],
        out_specs=vmem,
        scratch_shapes=[pltpu.VMEM((2 * ROWS, columns + capacity + LANES), jnp.float32)],
        compiler_params=params(),
        name="combine",
    )(starts, answer)


def on_device(
    clm_block,
    clm_cell,
    precip,
    evap_demand,
    root_share,
    sat_before,
    pressure,
    conductivity,
    porosity,
    freeze_state,
    land_mask,
):
    axes = ("gx", "gy")
    layers, columns = root_share.shape
    devices = lax.axis_size("gx") * lax.axis_size("gy")
    cells_x, cells_y = pressure.shape[1], pressure.shape[2]
    per_pair = columns // devices
    capacity = -(-(per_pair + per_pair // 2) // LANES) * LANES
    outgoing, starts = dispatch(
        clm_block, clm_cell, precip, evap_demand, root_share, sat_before, devices, capacity
    )
    flat = lax.all_to_all(outgoing.reshape(-1), axes, split_axis=0, concat_axis=0, tiled=True)

    fixed, low, high = prepare(conductivity, freeze_state, porosity, pressure)
    below, above = both_ways(low, high, "gx")
    to_left, to_right = pack(fixed, below, above)
    side_left, side_right = both_ways(to_left, to_right, "gy")
    fixed = (fixed, below, above, side_left, side_right)
    incoming = flat.reshape(outgoing.shape)

    source, low, high, order = scatter(incoming, land_mask, layers, cells_x, cells_y)
    below, above = both_ways(low, high, "gx")
    begun = begin(fixed, layers, cells_x, cells_y)
    source, below, above = source[None], below[None], above[None]
    to_left, to_right = pack(source, below, above)
    side_left, side_right = both_ways(to_left, to_right, "gy")
    source = (source, below, above, side_left, side_right)

    new_pressure, reply = newton(begun, source, incoming, order, layers, cells_x, cells_y)
    flat = lax.all_to_all(reply.reshape(-1), axes, split_axis=0, concat_axis=0, tiled=True)
    returned = combine(starts, flat.reshape(reply.shape), layers, columns, devices, capacity)
    return (new_pressure, returned)


def solution(mesh):
    columns = P(("gx", "gy"))
    layered = P(None, ("gx", "gy"))
    grid = P(None, "gx", "gy")
    return jax.shard_map(
        on_device,
        mesh=mesh,
        in_specs=(columns,) * 4 + (layered,) * 2 + (grid,) * 4 + (P("gx", "gy"),),
        out_specs=(grid, layered),
        check_vma=False,
    )
```

```python
import jax
import jax.numpy as jnp
from jax import lax
from jax.experimental import pallas as pl
from jax.experimental.pallas import tpu as pltpu
from jax.sharding import PartitionSpec as P

NEWTON = 2
SWEEPS = 4
OMEGA = 0.8
LANES = 128
ROWS = 8
HALO = 8
GROUPS = LANES // HALO


def params(mebibytes=16):
    return pltpu.CompilerParams(vmem_limit_bytes=mebibytes * 2**20)


def saturation(field):
    dryness = jnp.maximum(-field, 0.0)
    return lax.rsqrt(1.0 + dryness * dryness)


def frozen_factor(freeze_state):
    return jnp.where(freeze_state == 0, 1.0, jnp.where(freeze_state == 1, 0.2, 0.02)).astype(
        jnp.float32
    )


def window_tiles(capacity):
    return capacity // LANES


def scalar_rows(count):
    return -(-count // LANES)


def to_scalars(column, staged, scalars, sem):
    count = column.shape[0]
    for j in range(scalar_rows(count)):
        part = column[j * LANES : (j + 1) * LANES]
        shape = (part.shape[0], LANES)
        own = lax.broadcasted_iota(jnp.int32, shape, 0) == lax.broadcasted_iota(jnp.int32, shape, 1)
        staged[j : j + 1, :] = jnp.sum(jnp.where(own, part, 0), axis=0, keepdims=True)
    copy = pltpu.make_async_copy(staged, scalars, sem)
    copy.start()
    return copy


def scalar_at(scalars, index):
    if scalars.shape[0] == 1:
        return scalars[0, index]
    return scalars[index // LANES, index % LANES]


def dispatch_kernel(layers, devices, capacity):
    chunks = window_tiles(capacity)
    fields = layers + 1
    bounds = -(-(devices + 1) // ROWS) * ROWS

    def kernel(
        block_hbm, cell_hbm, precip_hbm, evap_hbm, root_hbm, sat_hbm,
        out, starts,
        packed, block, cell, precip, evap, root, sat, staged, sems,
    ):
        columns = root.shape[1]
        copies = [
            pltpu.make_async_copy(source, target, sems.at[i])
            for i, (source, target) in enumerate(
                (
                    (block_hbm, block),
                    (root_hbm, root),
                    (sat_hbm, sat),
                    (cell_hbm, cell),
                    (precip_hbm, precip),
                    (evap_hbm, evap),
                )
            )
        ]
        for copy in copies:
            copy.start()
        copies[0].wait()
        owner_row = lax.broadcasted_iota(jnp.int32, (bounds, LANES), 0)
        before = jnp.zeros((bounds, LANES), jnp.int32)
        for r in range(columns // LANES):
            before = before + (block[r : r + 1, :] < owner_row).astype(jnp.int32)
        before = jnp.sum(before.astype(jnp.float32), axis=1, keepdims=True)
        bounds_copy = to_scalars(before.astype(jnp.int32), staged, starts, sems.at[6])
        for copy in copies[1:]:
            copy.wait()

        def flux(tile, carry):
            span = pl.ds(pl.multiple_of(tile * LANES, LANES), LANES)
            s = sat[:, span]
            w = root[:, span] * s * s
            total = 0.25 + jnp.sum(w, axis=0, keepdims=True)
            uptake = w * (evap[pl.ds(tile, 1), :] / total)
            top = s[0:1]
            rain = precip[pl.ds(tile, 1), :] * (1.0 - top * top * top)
            packed[0:1, span] = rain - uptake[0:1]
            packed[1:layers, span] = -uptake[1:]
            packed[layers:fields, span] = cell[pl.ds(tile, 1), :].astype(jnp.float32)
            return carry

        lax.fori_loop(0, columns // LANES, flux, 0, unroll=16)
        bounds_copy.wait()
        lane = lax.broadcasted_iota(jnp.int32, (1, LANES), 1)

        def window(owner, carry):
            start = scalar_at(starts, owner)
            count = scalar_at(starts, owner + 1) - start
            base = pl.multiple_of((start // LANES) * LANES, LANES)
            shift = start % LANES
            near = lane < LANES - shift
            turned = [
                pltpu.roll(packed[:, pl.ds(base + t * LANES, LANES)], LANES - shift, 1)
                for t in range(chunks + 1)
            ]
            for t in range(chunks):
                moved = jnp.where(near, turned[t], turned[t + 1])
                row = (owner * chunks + t) * fields
                held = t * LANES + lane < count
                out[pl.ds(row, layers), :] = moved[0:layers]
                out[pl.ds(row + layers, 1), :] = jnp.where(held, moved[layers:fields], -1.0)
            return carry

        lax.fori_loop(0, devices, window, 0, unroll=4)

    return kernel


def dispatch(block, cell, precip, evap, root, sat, devices, capacity):
    layers, columns = root.shape
    fields = layers + 1
    rows = devices * window_tiles(capacity) * fields
    bounds = scalar_rows(-(-(devices + 1) // ROWS) * ROWS)
    vmem = pl.BlockSpec(memory_space=pltpu.VMEM)
    fold = (columns // LANES, LANES)
    return pl.pallas_call(
        dispatch_kernel(layers, devices, capacity),
        out_shape=(
            jax.ShapeDtypeStruct((rows, LANES), jnp.float32),
            jax.ShapeDtypeStruct((bounds, LANES), jnp.int32),
        ),
        in_specs=[pl.BlockSpec(memory_space=pltpu.HBM)] * 6,
        out_specs=(vmem, pl.BlockSpec(memory_space=pltpu.SMEM)),
        scratch_shapes=[
            pltpu.VMEM((2 * ROWS, columns + capacity + LANES), jnp.float32),
            pltpu.VMEM(fold, jnp.int32),
            pltpu.VMEM(fold, jnp.int32),
            pltpu.VMEM(fold, jnp.float32),
            pltpu.VMEM(fold, jnp.float32),
            pltpu.VMEM(root.shape, jnp.float32),
            pltpu.VMEM(root.shape, jnp.float32),
            pltpu.VMEM((bounds, LANES), jnp.int32),
            pltpu.SemaphoreType.DMA((7,)),
        ],
        compiler_params=params(),
        name="dispatch",
    )(
        *(
            pltpu.with_memory_space_constraint(a, pltpu.HBM)
            for a in (
                block.reshape(fold),
                cell.reshape(fold),
                precip.reshape(fold),
                evap.reshape(fold),
                root,
                sat,
            )
        )
    )


def scatter_kernel(layers, cells_x, cells_y, devices, batch):
    fields = layers + 1
    half = layers * cells_x

    def kernel(incoming, mask, out, low, high, order, total, spread, staged, used, sem):
        chunks = incoming.shape[0] // fields
        first_cells = incoming[pl.ds(layers, chunks, stride=fields), :][:, 0:1]
        used_copy = to_scalars((first_cells >= 0.0).astype(jnp.int32), staged, used, sem)
        each = chunks // devices

        def first(sender, carry):
            order[sender] = sender * each
            return carry

        lax.fori_loop(0, devices, first, 0, unroll=8)
        total[...] = jnp.zeros_like(total)
        row_x = lax.broadcasted_iota(jnp.int32, (cells_x, LANES), 0)
        row_y = lax.broadcasted_iota(jnp.int32, (cells_y, LANES), 0)

        def step(i, carry):
            onehots = []
            for b in range(batch):
                first = order[i * batch + b] * fields
                cell = incoming[pl.ds(first + layers, 1), :].astype(jnp.int32)
                x = cell // cells_y
                y = cell - x * cells_y
                x = jnp.where(cell < 0, -1, x)
                onehots.append((row_y == y).astype(jnp.float32).astype(jnp.bfloat16))
                here = row_x == x
                values = incoming[pl.ds(first, layers), :]
                big = values.astype(jnp.bfloat16).astype(jnp.float32)
                small = values - big
                span = slice(b * LANES, (b + 1) * LANES)
                for k in range(layers):
                    rows = slice(k * cells_x, (k + 1) * cells_x)
                    spread[rows, span] = jnp.where(here, big[k : k + 1], 0.0).astype(jnp.bfloat16)
                    rows = slice(half + k * cells_x, half + (k + 1) * cells_x)
                    spread[rows, span] = jnp.where(here, small[k : k + 1], 0.0).astype(
                        jnp.bfloat16
                    )
            onehot = jnp.concatenate(onehots, axis=1)
            total[...] += lax.dot_general(
                spread[...],
                onehot,
                (((1,), (1,)), ((), ())),
                preferred_element_type=jnp.float32,
            )
            return carry

        lax.fori_loop(0, devices // batch, step, 0)
        used_copy.wait()

        def listed(r, filled):
            c = r // (each - 1) * each + 1 + r % (each - 1)
            holds = scalar_at(used, c)
            order[jnp.where(holds > 0, filled, chunks - 1 - (r - (filled - devices)))] = c
            return filled + holds

        filled = jnp.int32(devices)
        if each > 1:
            filled = lax.fori_loop(0, chunks - devices, listed, filled, unroll=8)
        order[chunks] = filled
        lax.fori_loop(devices // batch, (filled + batch - 1) // batch, step, 0)
        land = mask[...].astype(jnp.float32)
        for k in range(layers):
            rows = slice(k * cells_x, (k + 1) * cells_x)
            lower = slice(half + k * cells_x, half + (k + 1) * cells_x)
            source = (total[rows, :] + total[lower, :]) * land
            out[k] = source
            low[k] = source[:HALO]
            high[k] = source[cells_x - HALO :]

    return kernel


def scatter(incoming, mask, layers, cells_x, cells_y, devices):
    chunks = incoming.shape[0] // (layers + 1)
    batch = max(b for b in (8, 4, 2, 1) if devices % b == 0)
    strip = jax.ShapeDtypeStruct((layers, HALO, cells_y), jnp.float32)
    vmem = pl.BlockSpec(memory_space=pltpu.VMEM)
    return pl.pallas_call(
        scatter_kernel(layers, cells_x, cells_y, devices, batch),
        out_shape=(
            jax.ShapeDtypeStruct((layers, cells_x, cells_y), jnp.float32),
            strip,
            strip,
            jax.ShapeDtypeStruct((chunks + 1,), jnp.int32),
        ),
        in_specs=[vmem, vmem],
        out_specs=(vmem, vmem, vmem, pl.BlockSpec(memory_space=pltpu.SMEM)),
        scratch_shapes=[
            pltpu.VMEM((2 * layers * cells_x, cells_y), jnp.float32),
            pltpu.VMEM((2 * layers * cells_x, batch * LANES), jnp.bfloat16),
            pltpu.VMEM((scalar_rows(chunks), LANES), jnp.int32),
            pltpu.SMEM((scalar_rows(chunks), LANES), jnp.int32),
            pltpu.SemaphoreType.DMA(()),
        ],
        compiler_params=params(),
        name="scatter",
    )(incoming, mask)


def both_ways(low_end, high_end, axis):
    count = lax.axis_size(axis)
    forward = [(i, i + 1) for i in range(count - 1)]
    backward = [(target, source) for source, target in forward]
    return lax.ppermute(high_end, axis, forward), lax.ppermute(low_end, axis, backward)


def packed_rows(layers, cells_x):
    tiles = layers * (cells_x + 2 * HALO) // ROWS
    return -(-tiles // GROUPS) * ROWS


def tile_places(layers, cells_x):
    tiles = (cells_x + 2 * HALO) // ROWS
    for index in range(layers * tiles):
        yield index // tiles, index % tiles, index // GROUPS, index % GROUPS


def pack_kernel(layers, cells_x, cells_y):
    lane_of = lambda: lax.broadcasted_iota(jnp.int32, (ROWS, LANES), 1)

    def kernel(middle, below, above, left, right):
        fields = middle.shape[0]
        lane = lane_of()
        last = cells_x // ROWS + 1

        def column(f, k, t, cols):
            if t == 0:
                return below[f, k, :, cols]
            if t == last:
                return above[f, k, :, cols]
            return middle[f, k, (t - 1) * ROWS : t * ROWS, cols]

        for f in range(fields):
            for out, cols, offset in (
                (left, slice(0, LANES), 0),
                (right, slice(cells_y - LANES, cells_y), LANES - HALO),
            ):
                held = {}
                for k, t, place, group in tile_places(layers, cells_x):
                    tile = column(f, k, t, cols)
                    turn = (group * HALO - offset) % LANES
                    tile = pltpu.roll(tile, turn, 1) if turn else tile
                    if group == 0:
                        held[place] = tile
                    else:
                        here = (lane >= group * HALO) & (lane < (group + 1) * HALO)
                        held[place] = jnp.where(here, tile, held[place])
                for place, tile in held.items():
                    out[f, place * ROWS : (place + 1) * ROWS, :] = tile

    return kernel


def pack(middle, below, above):
    fields, layers, cells_x, cells_y = middle.shape
    out = jax.ShapeDtypeStruct((fields, packed_rows(layers, cells_x), LANES), jnp.float32)
    vmem = pl.BlockSpec(memory_space=pltpu.VMEM)
    return pl.pallas_call(
        pack_kernel(layers, cells_x, cells_y),
        out_shape=(out, out),
        in_specs=[vmem] * 3,
        out_specs=(vmem, vmem),
        compiler_params=params(),
        name="pack",
    )(middle, below, above)


def prepare_kernel(conductivity, freeze, porosity, pressure, out, low, high):
    cells_x = out.shape[2]
    perm = conductivity[...] * frozen_factor(freeze[...])
    for f, value in enumerate((perm, porosity[...], pressure[...])):
        out[f] = value
        low[f] = value[:, :HALO]
        high[f] = value[:, cells_x - HALO :]


def prepare(conductivity, freeze, porosity, pressure):
    layers, cells_x, cells_y = pressure.shape
    strip = jax.ShapeDtypeStruct((3, layers, HALO, cells_y), jnp.float32)
    vmem = pl.BlockSpec(memory_space=pltpu.VMEM)
    return pl.pallas_call(
        prepare_kernel,
        out_shape=(jax.ShapeDtypeStruct((3, layers, cells_x, cells_y), jnp.float32), strip, strip),
        in_specs=[vmem] * 4,
        out_specs=(vmem,) * 3,
        compiler_params=params(),
        name="prepare",
    )(conductivity, freeze, porosity, pressure)


def gather_slots(order, incoming, table, split, reply, layers, cells_x, cells_y, turned):
    fields = layers + 1
    chunks = incoming.shape[0] // fields
    sub = lax.broadcasted_iota(jnp.int32, (ROWS, LANES), 0)
    row_x = lax.broadcasted_iota(jnp.int32, (cells_x, LANES), 0)
    row_y = lax.broadcasted_iota(jnp.int32, (cells_y, LANES), 0)
    across = cells_y // LANES
    groups = cells_x // ROWS * across
    half = split.shape[0] // 2
    together = max(b for b in (8, 4, 3, 2, 1) if chunks % b == 0)

    def looked_up(cell):
        cell = jnp.broadcast_to(cell, (ROWS, LANES))
        x = cell // cells_y
        y = cell - x * cells_y
        lane = y % LANES
        group = (x // ROWS) * across + y // LANES
        wanted = x % ROWS == sub
        rows = []
        for k in range(turned):
            value = jnp.zeros((ROWS, LANES), jnp.float32)
            for g in range(groups):
                first = HALO + g // across * ROWS
                tile = table[k, first : first + ROWS, g % across * LANES : (g % across + 1) * LANES]
                found = jnp.take_along_axis(tile, lane, axis=1, mode="promise_in_bounds")
                value = jnp.where(group == g, found, value)
            value = jnp.where(wanted, value, 0.0)
            rows.append(jnp.sum(value, axis=0, keepdims=True))
        return rows

    def body(i, carry):
        places = [order[i * together + b] for b in range(together)]
        cells = []
        onehots = []
        for c in places:
            cell = jnp.maximum(incoming[pl.ds(c * fields + layers, 1), :].astype(jnp.int32), 0)
            cells.append(cell)
            onehots.append((row_y == cell % cells_y).astype(jnp.float32).astype(jnp.bfloat16))
        product = jnp.dot(
            split[...], jnp.concatenate(onehots, axis=1), preferred_element_type=jnp.float32
        )
        for b, c in enumerate(places):
            rows = looked_up(cells[b])
            here = row_x == cells[b] // cells_y
            span = slice(b * LANES, (b + 1) * LANES)
            for k in range(layers - turned):
                upper = product[k * cells_x : (k + 1) * cells_x, span]
                lower = product[half + k * cells_x : half + (k + 1) * cells_x, span]
                found = jnp.where(here, upper + lower, 0.0)
                rows.append(jnp.sum(found, axis=0, keepdims=True))
            reply[pl.ds(c * layers, layers), :] = jnp.concatenate(rows, axis=0)
        return carry

    lax.fori_loop(0, (order[chunks] + together - 1) // together, body, 0)


class Stencil:
    def __init__(self, layers, cells_x, cells_y):
        self.layers, self.cells_x, self.cells_y = layers, cells_x, cells_y
        self.high_x, self.wide = cells_x + 2 * HALO, cells_y + LANES

    def up(self, v):
        return pltpu.roll(v, self.high_x - 1, 0)

    def down(self, v):
        return pltpu.roll(v, 1, 0)

    def right(self, v):
        return pltpu.roll(v, self.wide - 1, 1)

    def left(self, v):
        return pltpu.roll(v, 1, 1)

    def each_layer(self, do):
        for k in range(self.layers):
            do(k)

    def widen(self, dest, field, middle, low, high, side_left, side_right):
        layers, cells_x, cells_y = self.layers, self.cells_x, self.cells_y
        lane = lax.broadcasted_iota(jnp.int32, (ROWS, LANES), 1)
        dest[:, HALO : HALO + cells_x, :cells_y] = middle[field]
        dest[:, :HALO, :cells_y] = low[field]
        dest[:, HALO + cells_x :, :cells_y] = high[field]
        for k, t, place, group in tile_places(layers, cells_x):
            rows = slice(place * ROWS, (place + 1) * ROWS)
            turn = (LANES - HALO - group * HALO) % LANES
            a = side_left[field, rows, :]
            a = pltpu.roll(a, turn, 1) if turn else a
            turn = (-group * HALO) % LANES
            b = side_right[field, rows, :]
            b = pltpu.roll(b, turn, 1) if turn else b
            tile = jnp.where(lane < HALO, b, jnp.where(lane >= LANES - HALO, a, 0.0))
            dest[k, t * ROWS : (t + 1) * ROWS, cells_y:] = tile

    def faces(self, perm, tx, ty, tz):
        def face(a, b):
            joined = a + b
            return a * b / jnp.where(joined > 0.0, joined, 1.0)

        def still(k):
            a = perm[k]
            tx[k] = face(a, self.up(a))
            ty[k] = face(a, self.right(a))
            tz[k] = face(a, perm[min(k + 1, self.layers - 1)])

        self.each_layer(still)

    def linearize(self, pres, poro, stored, last_perm, tx, ty, tz, rel, gz, flow, weights, finish):
        ax, bx, ay, by, az, bz = weights
        layers = self.layers

        def relative(k):
            s = saturation(pres[k])
            rel[k] = s * s * s

        self.each_layer(relative)
        nothing = jnp.zeros((self.high_x, self.wide), jnp.float32)
        gz[0] = nothing
        flow[0] = nothing

        def vertical(k):
            r = rel[k]
            if k < layers - 1:
                g = tz[k] * (r + rel[k + 1])
                gz[k + 1] = g
                flow[k + 1] = g * (pres[k] - pres[k + 1] + 1.0)
            else:
                gz[k + 1] = nothing
                flow[k + 1] = last_perm * r

        self.each_layer(vertical)

        def linear(k):
            p = pres[k]
            r = rel[k]
            gx = tx[k] * (r + self.up(r))
            gy = ty[k] * (r + self.right(r))
            fx = gx * (p - self.up(p))
            fy = gy * (p - self.right(p))
            gxd = self.down(gx)
            gyd = self.left(gy)
            s = saturation(p)
            porous = poro[k]
            residual = porous * (s - stored[k])
            residual = residual + (fx - self.down(fx)) + (fy - self.left(fy))
            residual = residual + (flow[k + 1] - flow[k])
            gzd = gz[k]
            gzu = gz[k + 1]
            diagonal = porous * (jnp.maximum(-p, 0.0) * r)
            diagonal = diagonal + (gx + gxd) + (gy + gyd) + (gzu + gzd)
            diagonal = jnp.where(diagonal > 0.0, diagonal, 1.0)
            scale = OMEGA / diagonal
            ax[k] = scale * gx
            bx[k] = scale * gxd
            ay[k] = scale * gy
            by[k] = scale * gyd
            az[k] = scale * gzu
            bz[k] = scale * gzd
            finish(k, residual, scale)

        self.each_layer(linear)

    def sweeps(self, pres, weights, resid, update):
        ax, bx, ay, by, az, bz = weights
        layers = self.layers
        for sweep in range(SWEEPS - 1):
            old = sweep % 2
            new = 1 - old

            def smooth(k):
                u = update[old, k]
                v = (1.0 - OMEGA) * u - resid[k]
                v = v + ax[k] * self.up(u) + bx[k] * self.down(u)
                v = v + ay[k] * self.right(u) + by[k] * self.left(u)
                v = v + az[k] * update[old, min(k + 1, layers - 1)]
                v = v + bz[k] * update[old, max(k - 1, 0)]
                update[new, k] = v
                if sweep == SWEEPS - 2:
                    pres[k] = pres[k] + v

            self.each_layer(smooth)


def begin_kernel(grid):
    def kernel(
        fixed, low, high, side_left, side_right,
        pres, poro, stored, last_perm, tx, ty, tz, ax, bx, ay, by, az, bz, resid, scales,
        perm, rel, gz, flow,
    ):
        sides = (low, high, side_left, side_right)
        grid.widen(perm, 0, fixed, *sides)
        grid.widen(poro, 1, fixed, *sides)
        grid.widen(pres, 2, fixed, *sides)
        grid.faces(perm, tx, ty, tz)
        last_perm[...] = perm[grid.layers - 1]

        def keep(k):
            stored[k] = saturation(pres[k])

        grid.each_layer(keep)

        def finish(k, residual, scale):
            resid[k] = scale * residual
            scales[k] = scale

        grid.linearize(
            pres, poro, stored, last_perm[...], tx, ty, tz, rel, gz, flow,
            (ax, bx, ay, by, az, bz), finish,
        )

    return kernel


def begin(fixed, layers, cells_x, cells_y):
    grid = Stencil(layers, cells_x, cells_y)
    shape = (layers, grid.high_x, grid.wide)
    field = jax.ShapeDtypeStruct(shape, jnp.float32)
    plane = jax.ShapeDtypeStruct(shape[1:], jnp.float32)
    vmem = pl.BlockSpec(memory_space=pltpu.VMEM)
    outs = (field,) * 3 + (plane,) + (field,) * 11
    cells = layers * grid.high_x * grid.wide
    return pl.pallas_call(
        begin_kernel(grid),
        out_shape=outs,
        in_specs=[vmem] * 5,
        out_specs=(vmem,) * len(outs),
        scratch_shapes=[pltpu.VMEM(shape, jnp.float32)] * 2
        + [pltpu.VMEM((layers + 1,) + shape[1:], jnp.float32)] * 2,
        compiler_params=params(24),
        cost_estimate=pl.CostEstimate(
            flops=100 * cells, transcendentals=4 * cells, bytes_accessed=0
        ),
        name="begin",
    )(*fixed)


def newton_kernel(grid, turned):
    layers, cells_x, cells_y = grid.layers, grid.cells_x, grid.cells_y

    def kernel(
        pres0, poro, stored, last_perm, tx, ty, tz,
        ax0, bx0, ay0, by0, az0, bz0, resid0, scales,
        src, src_low, src_high, src_left, src_right, incoming, order,
        new_pressure, reply,
        source, pres, rel, gz, flow, ax, bx, ay, by, az, bz, resid, update, split,
    ):
        grid.widen(source, 0, src, src_low, src_high, src_left, src_right)

        def first(k):
            pres[k] = pres0[k]
            residual = resid0[k] - scales[k] * source[k]
            resid[k] = residual
            update[0, k] = -residual

        grid.each_layer(first)
        grid.sweeps(pres, (ax0, bx0, ay0, by0, az0, bz0), resid, update)
        weights = (ax, bx, ay, by, az, bz)
        for newton_step in range(1, NEWTON):

            def finish(k, residual, scale):
                residual = scale * (residual - source[k])
                resid[k] = residual
                update[0, k] = -residual

            grid.linearize(
                pres, poro, stored, last_perm[...], tx, ty, tz, rel, gz, flow, weights, finish
            )
            grid.sweeps(pres, weights, resid, update)

        half = split.shape[0] // 2
        for k in range(layers):
            p = pres[k, HALO : HALO + cells_x, :cells_y]
            new_pressure[k] = p
            s = saturation(p)
            if k < turned:
                rel[k, HALO : HALO + cells_x, :cells_y] = s
            else:
                row = (k - turned) * cells_x
                upper = s.astype(jnp.bfloat16)
                split[row : row + cells_x, :] = upper
                lower = (s - upper.astype(jnp.float32)).astype(jnp.bfloat16)
                split[half + row : half + row + cells_x, :] = lower
        gather_slots(order, incoming, rel, split, reply, layers, cells_x, cells_y, turned)

    return kernel


def newton(begun, source, incoming, order, layers, cells_x, cells_y):
    grid = Stencil(layers, cells_x, cells_y)
    turned = 2 * layers // 5
    chunks = incoming.shape[0] // (layers + 1)
    shape = (layers, grid.high_x, grid.wide)
    field = pltpu.VMEM(shape, jnp.float32)
    taller = pltpu.VMEM((layers + 1,) + shape[1:], jnp.float32)
    vmem = pl.BlockSpec(memory_space=pltpu.VMEM)
    return pl.pallas_call(
        newton_kernel(grid, turned),
        out_shape=(
            jax.ShapeDtypeStruct((layers, cells_x, cells_y), jnp.float32),
            jax.ShapeDtypeStruct((chunks * layers, LANES), jnp.float32),
        ),
        in_specs=[vmem] * 21 + [pl.BlockSpec(memory_space=pltpu.SMEM)],
        out_specs=(vmem, vmem),
        scratch_shapes=[field] * 3
        + [taller] * 2
        + [field] * 7
        + [
            pltpu.VMEM((2,) + shape, jnp.float32),
            pltpu.VMEM((2 * (layers - turned) * cells_x, cells_y), jnp.bfloat16),
        ],
        compiler_params=params(32),
        name="newton",
    )(*begun, *source, incoming, order)


def combine_kernel(layers, devices, capacity):
    chunks = window_tiles(capacity)

    def kernel(starts, answer, out, wide):
        lane = lax.broadcasted_iota(jnp.int32, (1, LANES), 1)

        def window(owner, carry):
            start = scalar_at(starts, owner)
            base = pl.multiple_of((start // LANES) * LANES, LANES)
            shift = start % LANES
            before = lane < shift
            row = owner * chunks * layers
            kept = wide[0:layers, pl.ds(base, LANES)]
            for t in range(chunks):
                turned = pltpu.roll(answer[pl.ds(row + t * layers, layers), :], shift, 1)
                wide[0:layers, pl.ds(base + t * LANES, LANES)] = jnp.where(before, kept, turned)
                kept = turned
            wide[0:layers, pl.ds(base + chunks * LANES, LANES)] = kept
            return carry

        lax.fori_loop(0, devices, window, 0, unroll=4)
        out[...] = wide[0:layers, : out.shape[1]]

    return kernel


def combine(starts, answer, layers, columns, devices, capacity):
    vmem = pl.BlockSpec(memory_space=pltpu.VMEM)
    return pl.pallas_call(
        combine_kernel(layers, devices, capacity),
        out_shape=jax.ShapeDtypeStruct((layers, columns), jnp.float32),
        in_specs=[pl.BlockSpec(memory_space=pltpu.SMEM), vmem],
        out_specs=vmem,
        scratch_shapes=[pltpu.VMEM((2 * ROWS, columns + capacity + LANES), jnp.float32)],
        compiler_params=params(),
        name="combine",
    )(starts, answer)


def on_device(
    clm_block,
    clm_cell,
    precip,
    evap_demand,
    root_share,
    sat_before,
    pressure,
    conductivity,
    porosity,
    freeze_state,
    land_mask,
):
    axes = ("gx", "gy")
    layers, columns = root_share.shape
    devices = lax.axis_size("gx") * lax.axis_size("gy")
    cells_x, cells_y = pressure.shape[1], pressure.shape[2]
    per_pair = columns // devices
    capacity = -(-(per_pair + per_pair // 2) // LANES) * LANES
    outgoing, starts = dispatch(
        clm_block, clm_cell, precip, evap_demand, root_share, sat_before, devices, capacity
    )
    flat = lax.all_to_all(outgoing.reshape(-1), axes, split_axis=0, concat_axis=0, tiled=True)

    fixed, low, high = prepare(conductivity, freeze_state, porosity, pressure)
    below, above = both_ways(low, high, "gx")
    to_left, to_right = pack(fixed, below, above)
    side_left, side_right = both_ways(to_left, to_right, "gy")
    fixed = (fixed, below, above, side_left, side_right)
    incoming = flat.reshape(outgoing.shape)

    source, low, high, order = scatter(incoming, land_mask, layers, cells_x, cells_y, devices)
    below, above = both_ways(low, high, "gx")
    begun = begin(fixed, layers, cells_x, cells_y)
    source, below, above = source[None], below[None], above[None]
    to_left, to_right = pack(source, below, above)
    side_left, side_right = both_ways(to_left, to_right, "gy")
    source = (source, below, above, side_left, side_right)

    new_pressure, reply = newton(begun, source, incoming, order, layers, cells_x, cells_y)
    flat = lax.all_to_all(reply.reshape(-1), axes, split_axis=0, concat_axis=0, tiled=True)
    returned = combine(starts, flat.reshape(reply.shape), layers, columns, devices, capacity)
    return (new_pressure, returned)


def solution(mesh):
    columns = P(("gx", "gy"))
    layered = P(None, ("gx", "gy"))
    grid = P(None, "gx", "gy")
    return jax.shard_map(
        on_device,
        mesh=mesh,
        in_specs=(columns,) * 4 + (layered,) * 2 + (grid,) * 4 + (P("gx", "gy"),),
        out_specs=(grid, layered),
        check_vma=False,
    )
```
